32 devices in a mesh: seq: 8 (over z, x), vocab: 4 (over y, core).
Axes of the slice: x: 2, y: 2, z: 4, core: 2. Of those that a mesh axis runs over, the one named last changes fastest.
Arguments:
- hidden: bfloat16 [2, 1024, 2048], P(None, 'seq'), may hold values from -6 to 6
- embedded: bfloat16 [2, 1024, 2048], P(None, 'seq'), may hold values from -6 to 6
- targets: int32 [2, 1024], P(None, 'seq'), may hold values from 0 to 51199
- main_mask: int32 [2, 1024], P(None, 'seq'), may hold values 0 or 1
- mtp_mask: int32 [2, 1024], P(None, 'seq'), may hold values from 0 to 1, as said below
- lengths: int32 [2], replicated, may hold values from 256 to 1024, as said below
- head_weight: bfloat16 [2048, 51200], P(None, ('seq', 'vocab')), may hold values from -7.6733202 to 7.6733202
- projection: bfloat16 [4096, 2048], P(None, 'vocab'), may hold values from -0.09375 to 0.09375
- main_gain: float32 [2048], replicated, may hold values from 0.5 to 1.5
- hidden_gain: float32 [2048], replicated, may hold values from 0.5 to 1.5
- embed_gain: float32 [2048], replicated, may hold values from 0.5 to 1.5
- mtp_gain: float32 [2048], replicated, may hold values from 0.5 to 1.5
Outputs:
- main_tokens: float32 [2, 1024], P(None, 'seq')
- mtp_tokens: float32 [2, 1024], P(None, 'seq')
- total_loss: float32 [], replicated
The draws below stay inside these ranges and needn't reach their ends.
Inputs may be any that keep to these rules, and one draw needn't show every extreme that they name: `mtp_mask`: 1 at every position that is a multiple of 128. `lengths`: the first sequence has length 1024.
All inputs are finite; a program needn't handle non-finite values. No bound on the sum of `main_mask` on one device may be relied on, other than what follows from the above.
Results may differ from the reference program's by a relative error of at most 0.0004.
The reference program's roundings to bfloat16 on the way (of `main_rows`, `previous`, `joined`, `mixed` and `mtp_rows`) count: a program that leaves them out, or rounds other values in their place, can miss the bound.
Values may be sent and summed in bfloat16 or wider, within the bound.
A program may use at most 128 MiB of HBM per device.

```python
import math
import jax
import jax.numpy as jnp
import numpy as np
from jax import lax

D = 2048
VOCAB = 51200
TOK_DEV = 128
MICRO = 2
SEQ = 1024


def draw_head_weight(key, part):
    key_base = jax.random.fold_in(key, 1)
    result_draw = jnp.clip(jax.random.normal(key_base, (D, VOCAB), jnp.float32), -6.0, 6.0) * (3.0 / math.sqrt(D))
    return result_draw.astype(jnp.bfloat16)


def draw_lengths(key, part):
    drawn = jax.random.randint(jax.random.fold_in(key, 11), (MICRO,), SEQ // 4, SEQ + 1).astype(jnp.int32)
    return drawn.at[0].set(SEQ)


def draw_mtp_mask(key, part):
    levels = jax.random.randint(jax.random.fold_in(key, 23), (MICRO, SEQ), 0, 4)
    position = jnp.arange(SEQ, dtype=jnp.int32)[None, :]
    return jnp.where((position % TOK_DEV == 0) | (levels < 3), 1, 0).astype(jnp.int32)


def touch_ends(values, stream_key, smallest, high):
    extent = values.shape
    place = [jax.random.randint(jax.random.fold_in(stream_key, axis), (), 0, extent[axis]) for axis in range(len(extent))]
    values = values.at[tuple(place)].set(smallest)
    longest = extent.index(max(extent))
    place[longest] = (place[longest] + 1) % extent[longest]
    return values.at[tuple(place)].set(high)


def block_levels(key, shape, shards, least, high):
    gain, own = 1.0, jax.random.fold_in(key, 6)
    for axis_at, blocks in shards:
        draws = jnp.exp(jax.random.uniform(jax.random.fold_in(own, axis_at), (blocks,), jnp.float32, least / len(shards), high / len(shards)))
        gain = gain * jnp.repeat(draws, shape[axis_at] // blocks).reshape([-1 if axis == axis_at else 1 for axis in range(len(shape))])
    return gain


def rank_bounds(count, slope):
    weights = [(1 << 20) // math.isqrt(standing ** slope) + 1 for standing in range(1, count + 1)]
    scale = 1 + sum(weights) // (1 << 30)
    return np.cumsum(np.array([max(1, weight // scale) for weight in weights]))


def ranked(key, dims, number_of, lean):
    table = rank_bounds(number_of, lean)
    ticket = jax.random.randint(jax.random.fold_in(key, 1), dims, 0, int(table[number_of - 1]))
    rank = jnp.searchsorted(jnp.asarray(table, jnp.int32), ticket, side="right")
    return jax.random.permutation(jax.random.fold_in(key, 2), number_of)[rank].astype(jnp.int32)


def scatter_about(key, shape, deviation, limit, cuts=(), kind=jnp.bfloat16):
    loudness = block_levels(key, shape, cuts, -0.22, 0.18) if cuts else 1.0
    result = jax.random.normal(key, shape, jnp.float32) * deviation * loudness
    return jnp.minimum(jnp.maximum(result, -limit), limit).astype(kind)


def setup_inputs(seed: int = 0) -> dict:
    streams_of = jax.random.split(jax.random.key(seed), 13)
    hidden = scatter_about(streams_of[0], (MICRO, SEQ, D), 1.0, 6.0, ((1, 8),))
    embedded = scatter_about(streams_of[1], (MICRO, SEQ, D), 1.0, 6.0, ((1, 8),))
    targets = touch_ends(ranked(streams_of[2], (MICRO, SEQ), VOCAB, 2), jax.random.fold_in(streams_of[2], 3), 0, VOCAB - 1).astype(jnp.int32)
    main_mask = touch_ends((jax.random.randint(streams_of[3], (MICRO, SEQ), 0, 4) < 3).astype(jnp.int32), jax.random.fold_in(streams_of[3], 1), 0, 1)
    mtp_mask = draw_mtp_mask(jax.random.fold_in(streams_of[12], 71), 0)
    lengths = draw_lengths(jax.random.fold_in(streams_of[12], 71), 0)
    head_weight = draw_head_weight(jax.random.fold_in(streams_of[12], 71), 0)
    projection = scatter_about(streams_of[7], (2 * D, D), (2 * D) ** -0.5, 0.09375, ((1, 4),))
    main_gain = jnp.clip(1.0 + 0.1 * jax.random.normal(streams_of[8], (D,), jnp.float32), 0.5, 1.5)
    hidden_gain = jnp.clip(1.0 + 0.1 * jax.random.normal(streams_of[9], (D,), jnp.float32), 0.5, 1.5)
    embed_gain = jnp.clip(1.0 + 0.1 * jax.random.normal(streams_of[10], (D,), jnp.float32), 0.5, 1.5)
    mtp_gain = jnp.clip(1.0 + 0.1 * jax.random.normal(streams_of[11], (D,), jnp.float32), 0.5, 1.5)
    return {"hidden": hidden, "embedded": embedded, "targets": targets, "main_mask": main_mask, "mtp_mask": mtp_mask, "lengths": lengths, "head_weight": head_weight, "projection": projection, "main_gain": main_gain, "hidden_gain": hidden_gain, "embed_gain": embed_gain, "mtp_gain": mtp_gain}


EPSILON = 1e-06
MTP_WEIGHT = 0.3

def normalize(values, gain_vec):
    values = values.astype(jnp.float32)
    mean_square = lax.optimization_barrier(jnp.mean(values * values, axis=-1, keepdims=True))
    return values * lax.rsqrt(mean_square + EPSILON) * gain_vec.astype(jnp.float32)

def cross_entropy(all_rows, wanted, head_weight):
    block_size = math.gcd(512, all_rows.shape[0])
    grouped = all_rows.reshape(-1, block_size, all_rows.shape[1])
    grouped_ids = wanted.reshape(-1, block_size)

    def one_block(block_pair):
        block_rows, block_ids = block_pair
        logits = jnp.dot(block_rows, head_weight, preferred_element_type=jnp.float32)
        highest = lax.optimization_barrier(jnp.max(logits, axis=1))
        exp_total = lax.optimization_barrier(jnp.sum(jnp.exp(logits - highest[:, None]), axis=1))
        target_logit = jnp.take_along_axis(logits, block_ids[:, None].astype(jnp.int32), axis=1)[:, 0]
        return highest + jnp.log(exp_total) - target_logit
    return lax.map(one_block, (grouped, grouped_ids)).reshape(-1)

def reference(hidden, embedded, targets, main_mask, mtp_mask, lengths, head_weight, projection, main_gain, hidden_gain, embed_gain, mtp_gain):
    batches, seq_len, model_width = hidden.shape
    positions = jnp.arange(seq_len, dtype=jnp.int32)[None, :]
    length_col = lengths[:, None]
    keep_main = ((main_mask == 1) & (positions + 1 < length_col)).astype(jnp.float32)
    keep_mtp = ((mtp_mask == 1) & (positions >= 1) & (positions + 1 < length_col)).astype(jnp.float32)
    main_rows = normalize(hidden, main_gain).astype(jnp.bfloat16).reshape(-1, model_width)
    previous = jnp.concatenate([jnp.zeros((batches, 1, model_width), hidden.dtype), hidden[:, :-1, :]], axis=1)
    joined = jnp.concatenate([normalize(previous, hidden_gain), normalize(embedded, embed_gain)], axis=2)
    joined = joined.astype(jnp.bfloat16).reshape(-1, 2 * model_width)
    mixed = jnp.dot(joined, projection, preferred_element_type=jnp.float32).astype(jnp.bfloat16)
    mtp_rows = normalize(mixed, mtp_gain).astype(jnp.bfloat16)
    flat_targets = targets.reshape(-1)
    main_losses = cross_entropy(main_rows, flat_targets, head_weight).reshape(batches, seq_len)
    mtp_losses = cross_entropy(mtp_rows, flat_targets, head_weight).reshape(batches, seq_len)
    main_tokens = keep_main * main_losses
    mtp_tokens = keep_mtp * mtp_losses
    total_loss = jnp.sum(main_tokens) / jnp.maximum(jnp.sum(keep_main), 1.0) + MTP_WEIGHT * jnp.sum(mtp_tokens) / jnp.maximum(jnp.sum(keep_mtp), 1.0)
    return (main_tokens, mtp_tokens, total_loss)
```

```python
import functools

import jax
import jax.numpy as jnp
from jax import lax
from jax.experimental import pallas as pl
from jax.experimental.pallas import tpu as pltpu
from jax.sharding import PartitionSpec as P

EPSILON = 1e-06
MTP_WEIGHT = 0.3
CHUNK = 256
SHARE = 8
ROWS = (((1,), (1,)), ((), ()))
MESH = pl.DeviceIdType.MESH


def from_behind(block, axis, distance):
    devices = range(lax.axis_size(axis))
    route = [(i - distance, i) for i in devices if i - distance in devices]
    return lax.ppermute(block, axis, route)


def normalize(values, gain_vec):
    values = values.astype(jnp.float32)
    mean_square = jnp.mean(values * values, axis=-1, keepdims=True)
    return values * lax.rsqrt(mean_square + EPSILON) * gain_vec


def join_stats(earlier, latter):
    highest = jnp.maximum(earlier[0], latter[0])
    exp_total = earlier[1] * jnp.exp(earlier[0] - highest) + latter[1] * jnp.exp(
        latter[0] - highest
    )
    return (highest, exp_total, earlier[2] + latter[2])


def seq_perm(value, bit):
    pairs = [(i, i ^ (1 << bit)) for i in range(lax.axis_size("seq"))]
    return lax.ppermute(value, "seq", pairs)


def vocab_perm(value, bit):
    pairs = [(i, i ^ (1 << bit)) for i in range(lax.axis_size("vocab"))]
    return lax.ppermute(value, "vocab", pairs)


def bits_of(axis):
    return list(reversed(range(lax.axis_size(axis).bit_length() - 1)))


def slot_masks(axis):
    masks = [0]
    for bit in bits_of(axis):
        masks = masks + [mask | (1 << bit) for mask in masks]
    return jnp.array(masks, jnp.int32)


def gather_pieces(own):
    pieces = [own]
    for bit in bits_of("seq"):
        held = pieces[0] if len(pieces) == 1 else jnp.concatenate(pieces, axis=0)
        pieces.append(seq_perm(held, bit))
    return pieces


def head_kernel(masks, at_ref, order_ref, *refs):
    blocks = refs[: len(masks)]
    gain_ref, local_ref, w_ref, out_ref, rows_ref = refs[len(masks) :]
    rows, width = rows_ref.shape
    part = blocks[0].shape[2]
    values = [block[0].astype(jnp.float32) for block in blocks]
    square = sum(jnp.sum(v * v, axis=1, keepdims=True) for v in values)
    scale = lax.rsqrt(square / width + EPSILON)
    for mask, value in zip(masks, values):
        place = pl.ds(pl.multiple_of((at_ref[0] ^ mask) * part, part), part)
        rows_ref[:, place] = (value * scale * gain_ref[:, place]).astype(jnp.bfloat16)
    wanted = local_ref[0]
    cols = w_ref.shape[1]
    stats = None
    for start in range(0, cols, CHUNK):
        stop = min(start + CHUNK, cols)
        logits = jnp.dot(
            rows_ref[...], w_ref[:, start:stop], preferred_element_type=jnp.float32
        )
        ids = lax.broadcasted_iota(jnp.int32, logits.shape, 1) + start
        highest = jnp.max(logits, axis=1, keepdims=True)
        total = jnp.sum(jnp.exp(logits - highest), axis=1, keepdims=True)
        picked = jnp.sum(jnp.where(ids == wanted, logits, 0.0), axis=1, keepdims=True)
        fresh = (highest, total, picked)
        stats = fresh if stats is None else join_stats(stats, fresh)
    lane = lax.broadcasted_iota(jnp.int32, (rows, 128), 1)
    packed = jnp.where(lane == 0, stats[0], jnp.where(lane == 1, stats[1], stats[2]))
    out_ref[0] = packed.T[:8]


def head_stats(masks, at, order, blocks, gain, local, head_weight):
    count, rows, part = blocks[0].shape
    width, cols = head_weight.shape
    flops = 2 * count * rows * width * cols
    return pl.pallas_call(
        functools.partial(head_kernel, masks),
        out_shape=jax.ShapeDtypeStruct((count, 8, rows), jnp.float32),
        grid_spec=pltpu.PrefetchScalarGridSpec(
            num_scalar_prefetch=2,
            grid=(count,),
            in_specs=[pl.BlockSpec((1, rows, part), lambda i, at, order: (i, 0, 0)) for _ in blocks]
            + [
                pl.BlockSpec((1, width), lambda i, at, order: (0, 0)),
                pl.BlockSpec((1, rows, 1), lambda i, at, order: (i, 0, 0)),
                pl.BlockSpec((width, cols), lambda i, at, order: (0, 0)),
            ],
            out_specs=pl.BlockSpec((1, 8, rows), lambda i, at, order: (order[i], 0, 0)),
            scratch_shapes=[pltpu.VMEM((rows, width), jnp.bfloat16)],
        ),
        compiler_params=pltpu.CompilerParams(vmem_limit_bytes=48 * 2**20),
        cost_estimate=pl.CostEstimate(
            flops=flops, bytes_accessed=2 * (width * cols + count * rows * width), transcendentals=count * rows * cols
        ),
    )(at, order, *blocks, gain.reshape(1, -1), local, head_weight)


def join_all(stats):
    highest = jnp.max(stats[:, 0], axis=0)
    total = jnp.sum(stats[:, 1] * jnp.exp(stats[:, 0] - highest), axis=0)
    return jnp.stack([highest, total, jnp.sum(stats[:, 2], axis=0)])


def finish(main_stats, mtp_stats):
    packed = jnp.concatenate([main_stats[:, :3], mtp_stats[:, :3]], axis=2)
    mine = lax.all_to_all(packed, "seq", 0, 0, tiled=True)
    joined = join_all(lax.all_gather(join_all(mine), "vocab"))
    return joined[0] + jnp.log(joined[1]) - joined[2]


def shards(
    hidden,
    embedded,
    targets,
    main_mask,
    mtp_mask,
    lengths,
    head_weight,
    projection,
    main_gain,
    hidden_gain,
    embed_gain,
    mtp_gain,
):
    batches, seq_len, model_width = hidden.shape
    rows = batches * seq_len
    seq_index = lax.axis_index("seq")
    vocab_index = lax.axis_index("vocab")
    vocab_count = lax.axis_size("vocab")
    cols = head_weight.shape[1]

    incoming = from_behind(hidden[:, seq_len - 1 :, :], "seq", 1)

    core = vocab_index & 1
    half = model_width // 2
    flat = hidden.reshape(1, rows, model_width)
    mine = lax.dynamic_slice_in_dim(flat, core * half, half, axis=2)
    other = lax.dynamic_slice_in_dim(flat, (1 - core) * half, half, axis=2)
    main_pieces = gather_pieces(mine)
    main_other = [other] + [vocab_perm(piece, 0) for piece in main_pieces[1:]]
    main_blocks = [jnp.concatenate(p, axis=0) for p in (main_pieces, main_other)]

    wanted = jnp.concatenate(gather_pieces(targets.reshape(1, rows)), axis=0)
    local = (wanted - (seq_index * vocab_count + vocab_index) * cols)[:, :, None]

    previous = jnp.concatenate([incoming, hidden[:, : seq_len - 1, :]], axis=1)
    joined = jnp.concatenate(
        [normalize(previous, hidden_gain), normalize(embedded, embed_gain)], axis=2
    )
    joined = joined.astype(jnp.bfloat16).reshape(rows, 2 * model_width)
    mixed = jnp.dot(joined, projection, preferred_element_type=jnp.float32).astype(jnp.bfloat16)
    masks = [0]
    held = [gather_pieces(mixed[None])]
    for bit in bits_of("vocab"):
        masks = masks + [mask | (1 << bit) for mask in masks]
        held = held + [[vocab_perm(piece, bit) for piece in pieces] for pieces in held]
    mtp_blocks = [jnp.concatenate(pieces, axis=0) for pieces in held]

    order = slot_masks("seq") ^ seq_index
    with jax.named_scope("mainhead"):
        main_stats = head_stats((0, 1), core[None], order, main_blocks, main_gain, local, head_weight)
    mtp_stats = head_stats(
        tuple(masks), vocab_index[None], order, mtp_blocks, mtp_gain, local, head_weight
    )

    positions = seq_index * seq_len + lax.broadcasted_iota(jnp.int32, (batches, seq_len), 1)
    inside = positions + 1 < lengths[:, None]
    keep_main = ((main_mask == 1) & inside).astype(jnp.float32)
    keep_mtp = ((mtp_mask == 1) & (positions >= 1) & inside).astype(jnp.float32)
    losses = finish(main_stats, mtp_stats).reshape(2, batches, seq_len)
    main_tokens = keep_main * losses[0]
    mtp_tokens = keep_mtp * losses[1]
    sums = jnp.stack(
        [jnp.sum(main_tokens), jnp.sum(mtp_tokens), jnp.sum(keep_main), jnp.sum(keep_mtp)]
    )
    for bit in bits_of("seq"):
        sums = sums + seq_perm(sums, bit)
    total_loss = sums[0] / jnp.maximum(sums[2], 1.0) + MTP_WEIGHT * sums[1] / jnp.maximum(
        sums[3], 1.0
    )
    return (main_tokens, mtp_tokens, total_loss)


def line_rank(place, count, j):
    near = jnp.minimum(place, count - 1 - place)
    step = (j + 1) // 2
    close = place + step * (1 - 2 * (j % 2))
    far = jnp.where(place < count - 1 - place, j, count - 1 - j)
    return jnp.where(j <= 2 * near, close, far)


def rms_rows(values, gain, width):
    square = jnp.sum(values * values, axis=1, keepdims=True)
    return values * lax.rsqrt(square / width + EPSILON) * gain


def pick(table, index):
    value = table[0]
    for at, entry in enumerate(table[1:], 1):
        value = jnp.where(index == at, entry, value)
    return value


def plan(depth, ax, az, ay, bz, bx, tz, ty, tx):
    bind = functools.partial
    steps = [
        ((0, 0, 0), [ax], [bind(az, 1, 0), bind(bz, 1)]),
        ((1, 0, 0), [bind(ty, 0)], [bind(tz, 1)]),
        ((0, 0, 1), [bind(az, 1, 1), bind(ay, 0, 1), bind(bx, 0)], [bind(az, 2, 0), bind(bz, 2)]),
    ]
    for j in range(1, depth):
        steps += [
            ((0, j, 0), [bind(ay, j, 0)], [bind(ty, j)]),
            ((1, j, 0), [], [bind(az, j + 1, 1)] if j + 1 < depth else []),
            ((1, j - 1, 1), [bind(tx, j - 1)], [bind(tz, j + 1)] if j + 1 < depth else []),
            (
                (0, j, 1),
                [bind(ay, j, 1), bind(bx, j)],
                [bind(az, j + 2, 0), bind(bz, j + 2)] if j + 2 < depth else [],
            ),
        ]
    steps.append(((1, depth - 1, 1), [bind(tx, depth - 1)], []))
    return [block for block, _, _ in steps], [group for _, *groups in steps for group in groups]


def fused_kernel(
    sizes,
    hidden,
    embedded,
    weight,
    projection,
    targets,
    main_mask,
    mtp_mask,
    lengths,
    main_gain,
    hidden_gain,
    embed_gain,
    mtp_gain,
    main_out,
    mtp_out,
    total_out,
    grid,
    wide,
    proj,
    own_hidden,
    own_embedded,
    joined,
    mixed,
    last,
    behind,
    wanted,
    rows,
    want,
    highs,
    sums,
    picks,
    packed,
    gathered,
    tokens,
    load_sem,
    send_sem,
    recv_sem,
    small_send,
    small_recv,
    stat_send,
    stat_recv,
):
    depth, spots = sizes
    count = depth * 2
    s, v = lax.axis_index("seq"), lax.axis_index("vocab")
    vocab = lax.axis_size("vocab")
    z, x, y, c = s // 2, s % 2, v // 2, v % 2
    height, width = rows.shape
    half = width // 2
    feature = mixed.shape[1]
    cols = weight.shape[0]
    split = spots
    turn_cols = CHUNK * (wide.shape[0] // CHUNK // 2)
    columns_of = pl.ds(pl.multiple_of(c * cols, 16), cols)

    def place(z_at, x_at, y_at, c_at):
        return (z_at * 2 + x_at, y_at * 2 + c_at)

    mine = pl.ds(pl.multiple_of(c * height, height), height)
    loads = [
        pltpu.make_async_copy(hidden.at[mine], grid.at[s], load_sem.at[0]),
        pltpu.make_async_copy(hidden, own_hidden, load_sem.at[1]),
        pltpu.make_async_copy(embedded, own_embedded, load_sem.at[2]),
        pltpu.make_async_copy(projection, proj, load_sem.at[3]),
        pltpu.make_async_copy(weight, wide.at[columns_of], load_sem.at[4]),
    ]
    for load in loads:
        load.start()

    barrier = pltpu.get_barrier_semaphore()
    devices = count * vocab
    me = s * vocab + v

    def greet(i, carry):
        other = lax.rem(me + i, devices)
        pl.semaphore_signal(
            barrier, inc=1, device_id=(other // vocab, lax.rem(other, vocab)), device_id_type=MESH
        )
        return carry

    lax.fori_loop(1, devices, greet, 0)
    wanted[s] = jnp.broadcast_to(targets[pl.ds(c, 1), :], wanted.shape[1:])
    loads[1].wait()
    for b in range(2):
        last[b : b + 1, :] = own_hidden[(b + 1) * height - 1 : (b + 1) * height, :]
    pl.semaphore_wait(barrier, devices - 1)

    def chunk(kind, at, part):
        if kind == "b":
            return grid.at[at, pl.ds(split, height - split)], count * 2 + at
        columns = pl.ds(pl.multiple_of(part * half, half), half)
        if kind == "a":
            return grid.at[at, pl.ds(0, split), columns], at * 2 + part
        return grid.at[count + at, :, columns], count * 3 + at * 2 + part

    def send(go, kind, at, part, way, device, when=None):
        ref, index = chunk(kind, at, part)
        copy = pltpu.make_async_remote_copy(
            src_ref=ref,
            dst_ref=ref,
            send_sem=send_sem.at[way, index],
            recv_sem=recv_sem.at[index],
            device_id=device,
            device_id_type=MESH,
        )
        act = copy.start if go else copy.wait_send
        if when is None:
            act()
        else:
            pl.when(when)(act)

    def arrive(go, kind, at, part):
        if not go:
            return
        ref, index = chunk(kind, at, part)
        pltpu.make_async_remote_copy(
            src_ref=ref,
            dst_ref=ref,
            send_sem=send_sem.at[0, index],
            recv_sem=recv_sem.at[index],
            device_id=(s, v),
            device_id_type=MESH,
        ).wait_recv()

    def z_both(go, kind, at, part):
        send(go, kind, at, part, 0, place(z + 1, x, y, c), z + 1 < depth)
        send(go, kind, at, part, 1, place(z - 1, x, y, c), z > 0)

    def z_on(go, kind, at, part, origin):
        onward = jnp.where(origin < z, z + 1, z - 1)
        when = (onward >= 0) & (onward < depth)
        send(go, kind, at, part, 0, place(onward, x, y, c), when)

    def x_over(go, kind, at, part):
        send(go, kind, at, part, 2, place(z, 1 - x, y, c))

    def y_over(go, kind, at, part):
        send(go, kind, at, part, 3, place(z, x, 1 - y, c))

    def at_of(jz, jx):
        return line_rank(z, depth, jz) * 2 + lax.rem(x + jx, 2)

    def ax(go):
        arrive(go, "a", at_of(0, 1), y)
        z_both(go, "a", at_of(0, 1), y)
        y_over(go, "a", at_of(0, 1), y)

    def az(jz, jx, go):
        arrive(go, "a", at_of(jz, jx), y)
        z_on(go, "a", at_of(jz, jx), y, line_rank(z, depth, jz))
        y_over(go, "a", at_of(jz, jx), y)

    def ay(jz, jx, go):
        arrive(go, "a", at_of(jz, jx), 1 - y)

    def bz(jz, go):
        arrive(go, "b", at_of(jz, 0), 0)
        z_on(go, "b", at_of(jz, 0), 0, line_rank(z, depth, jz))
        x_over(go, "b", at_of(jz, 0), 0)

    def bx(jz, go):
        arrive(go, "b", at_of(jz, 1), 0)

    def tz(jz, go):
        arrive(go, "t", at_of(jz, 0), y)
        x_over(go, "t", at_of(jz, 0), y)
        y_over(go, "t", at_of(jz, 0), y)
        z_on(go, "t", at_of(jz, 0), y, line_rank(z, depth, jz))

    def ty(jz, go):
        arrive(go, "t", at_of(jz, 0), 1 - y)
        x_over(go, "t", at_of(jz, 0), 1 - y)

    def tx(jz, go):
        arrive(go, "t", at_of(jz, 1), y)
        arrive(go, "t", at_of(jz, 1), 1 - y)

    def own_main(go):
        z_both(go, "a", s, y)
        x_over(go, "a", s, y)
        z_both(go, "b", s, 0)
        x_over(go, "b", s, 0)

    def own_mixed(go):
        x_over(go, "t", s, y)
        y_over(go, "t", s, y)
        z_both(go, "t", s, y)

    tail = pltpu.make_async_remote_copy(
        src_ref=last,
        dst_ref=behind,
        send_sem=small_send.at[0],
        recv_sem=small_recv.at[0],
        device_id=(s + 1, v),
        device_id_type=MESH,
    )
    pl.when(s + 1 < count)(tail.start)
    loads[0].wait()
    own_main(True)

    def target_copy(i):
        return pltpu.make_async_remote_copy(
            src_ref=wanted.at[s],
            dst_ref=wanted.at[s],
            send_sem=small_send.at[1 + i],
            recv_sem=small_recv.at[1 + s],
            device_id=(lax.rem(s + i, count), v),
            device_id_type=MESH,
        )

    for i in range(1, count):
        target_copy(i).start()
    swap = pltpu.make_async_remote_copy(
        src_ref=weight,
        dst_ref=wide.at[columns_of],
        send_sem=small_send.at[0 + 1 + count],
        recv_sem=small_recv.at[1 + count],
        device_id=place(z, x, y, 1 - c),
        device_id_type=MESH,
    )
    swap.start()

    loads[2].wait()
    slab = 32

    def norm_embedded(i, carry):
        part = pl.ds(pl.multiple_of(i * slab, slab), slab)
        value = own_embedded[part, :].astype(jnp.float32)
        joined[part, width:] = rms_rows(value, embed_gain[...], width).astype(jnp.bfloat16)
        return carry

    lax.fori_loop(0, 2 * height // slab, norm_embedded, 0)

    @pl.when(s == 0)
    def _():
        behind[...] = jnp.zeros_like(behind)

    @pl.when(s > 0)
    def _():
        tail.wait_recv()

    first = rms_rows(behind[...].astype(jnp.float32), hidden_gain[...], width)
    for b in range(2):
        value = own_hidden[b * height : (b + 1) * height, :].astype(jnp.float32)
        value = pltpu.roll(rms_rows(value, hidden_gain[...], width), 1, 0)
        row = lax.broadcasted_iota(jnp.int32, value.shape, 0)
        value = jnp.where(row == 0, first[b : b + 1, :], value)
        joined[b * height : (b + 1) * height, :width] = value.astype(jnp.bfloat16)
    loads[3].wait()
    mixed[...] = jnp.dot(
        joined[...], proj[...], preferred_element_type=jnp.float32
    ).astype(jnp.bfloat16)
    place_of = pl.ds(pl.multiple_of(v * feature, feature), feature)
    other = pl.ds(pl.multiple_of((1 - c) * height, height), height)
    trade = pltpu.make_async_remote_copy(
        src_ref=mixed.at[other],
        dst_ref=grid.at[count + s, :, place_of],
        send_sem=small_send.at[2 + count],
        recv_sem=small_recv.at[2 + count],
        device_id=place(z, x, y, 1 - c),
        device_id_type=MESH,
    )
    trade.start()
    grid[count + s, :, place_of] = mixed[mine, :]
    trade.wait_recv()
    own_mixed(True)
    loads[4].wait()

    order, events = plan(depth, ax, az, ay, bz, bx, tz, ty, tx)
    codes = [head * count + jz * 2 + jx for head, jz, jx in order]
    first_swap = 0
    lane = lax.broadcasted_iota(jnp.int32, (height, 128), 1)

    def stat_copy(head, at, i):
        return pltpu.make_async_remote_copy(
            src_ref=packed.at[head * count + at],
            dst_ref=gathered.at[head, c * count * 2 + s * 2 + y],
            send_sem=stat_send.at[head],
            recv_sem=stat_recv.at[head],
            device_id=(at, lax.rem(v + i, vocab)),
            device_id_type=MESH,
        )

    def unit(step, carry):
        code = pick(codes, step // 2)
        turn = lax.rem(step, 2)
        head, jz, jx = code // count, lax.rem(code, count) // 2, lax.rem(code, 2)
        at = line_rank(z, depth, jz) * 2 + lax.rem(x + jx, 2)
        for index, group in enumerate(events):
            if group:

                @pl.when(step == index)
                def _(group=group):
                    for event in group:
                        event(True)

        @pl.when(step == first_swap)
        def _():
            swap.wait_recv()

        @pl.when(turn == 0)
        def _():
            gain = jnp.where(head == 0, main_gain[...], mtp_gain[...])

            def norm(i, carry):
                part = pl.ds(pl.multiple_of(i * slab, slab), slab)
                value = grid[head * count + at, part, :].astype(jnp.float32)
                rows[part, :] = rms_rows(value, gain, width).astype(jnp.bfloat16)
                return carry

            lax.fori_loop(0, height // slab, norm, 0)
            line = wanted[at, 0:1, :].astype(jnp.float32)
            want[...] = jnp.broadcast_to(line, (128, height)).T.astype(jnp.int32)
            highs[...] = jnp.full_like(highs, -1e30)
            sums[...] = jnp.zeros_like(sums)
            picks[...] = jnp.zeros_like(picks)

        begin = pl.multiple_of(turn * turn_cols, CHUNK)
        relative = want[...] - lane - (s * vocab + y * 2) * cols - begin

        def add(state, start, size, columns):
            high, total, picked = state
            logits = lax.dot_general(
                rows[...], wide[columns, :], ROWS, preferred_element_type=jnp.float32
            )
            tiles = [logits[:, k : k + 128] for k in range(0, size, 128)]
            higher = functools.reduce(jnp.maximum, tiles, high)
            total = total * jnp.exp(high - higher)
            for k, tile in enumerate(tiles):
                total = total + jnp.exp(tile - higher)
                picked = picked + jnp.where(relative == start + 128 * k, tile, 0.0)
            return higher, total, picked

        state = highs[...], sums[...], picks[...]
        for start in range(0, turn_cols, CHUNK):
            state = add(state, start, CHUNK, pl.ds(pl.multiple_of(begin + start, CHUNK), CHUNK))

        @pl.when(turn == 0)
        def _():
            highs[...], sums[...], picks[...] = state

        @pl.when(turn == 1)
        def _():
            ended = state
            for start in range(2 * turn_cols, 2 * cols, CHUNK):
                size = min(CHUNK, 2 * cols - start)
                ended = add(ended, start - turn_cols, size, pl.ds(start, size))
            high, total, picked = ended
            top = jnp.max(high, axis=1, keepdims=True)
            added = jnp.sum(total * jnp.exp(high - top), axis=1, keepdims=True)
            found = jnp.sum(picked, axis=1, keepdims=True)
            block = jnp.where(lane == 0, top, jnp.where(lane == 1, added, found))
            packed[head * count + at] = block.T[:8]
            for i in range(1, vocab):
                stat_copy(head, at, i).start()

            @pl.when(at != s)
            def _():
                stat_copy(head, at, 0).start()

            @pl.when(at == s)
            def _():
                pltpu.make_async_copy(
                    packed.at[head * count + at],
                    gathered.at[head, c * count * 2 + s * 2 + y],
                    stat_recv.at[head],
                ).start()

        return carry

    for i in range(1, count):
        source = lax.rem(s + i, count)
        pltpu.make_async_remote_copy(
            src_ref=wanted.at[source],
            dst_ref=wanted.at[source],
            send_sem=small_send.at[1 + i],
            recv_sem=small_recv.at[1 + source],
            device_id=(s, v),
            device_id_type=MESH,
        ).wait_recv()
    lax.fori_loop(0, 2 * len(order), unit, 0)

    lengths_of = [lengths[0], lengths[1]]
    position = s * height + lax.broadcasted_iota(jnp.int32, (1, height), 1)
    loss = [[None, None], [None, None]]
    group = count * 2
    for head in range(2):
        whole = gathered.at[head]
        pltpu.make_async_copy(whole, whole, stat_recv.at[head]).wait()
        for b in range(2):
            part = gathered[head, b * group : (b + 1) * group, 0:3, :]
            tops = part[:, 0, :]
            top = jnp.max(tops, axis=0, keepdims=True)
            added = jnp.sum(part[:, 1, :] * jnp.exp(tops - top), axis=0, keepdims=True)
            found = jnp.sum(part[:, 2, :], axis=0, keepdims=True)
            loss[head][b] = top + jnp.log(added) - found
    lines = [jnp.zeros((1, height), jnp.float32)] * 4
    for b in range(2):
        inside = position + 1 < lengths_of[b]
        keep = [
            jnp.where((main_mask[b : b + 1, :] == 1) & inside, 1.0, 0.0),
            jnp.where((mtp_mask[b : b + 1, :] == 1) & (position >= 1) & inside, 1.0, 0.0),
        ]
        for head, out in enumerate((main_out, mtp_out)):
            kept = keep[head] * loss[head][b]
            out[b : b + 1, :] = kept
            lines[head] = lines[head] + kept
            lines[2 + head] = lines[2 + head] + keep[head]
    sub = lax.broadcasted_iota(jnp.int32, (8, height), 0)
    tile = jnp.zeros((8, height), jnp.float32)
    for at, line in enumerate(lines):
        tile = jnp.where(sub == at, line, tile)
    tokens[s] = tile

    def token_copy(i):
        return pltpu.make_async_remote_copy(
            src_ref=tokens.at[s],
            dst_ref=tokens.at[s],
            send_sem=small_send.at[3 + count + i],
            recv_sem=small_recv.at[3 + count + s],
            device_id=(lax.rem(s + i, count), v),
            device_id_type=MESH,
        )

    for i in range(1, count):
        token_copy(i).start()
    for i in range(1, count):
        source = lax.rem(s + i, count)
        pltpu.make_async_remote_copy(
            src_ref=tokens.at[source],
            dst_ref=tokens.at[source],
            send_sem=small_send.at[3 + count + i],
            recv_sem=small_recv.at[3 + count + source],
            device_id=(s, v),
            device_id_type=MESH,
        ).wait_recv()
    added = tokens[0]
    for i in range(1, count):
        added = added + tokens[i]
    added = jnp.sum(added, axis=1, keepdims=True)
    total_out[...] = added[0:1] / jnp.maximum(added[2:3], 1.0) + MTP_WEIGHT * added[
        1:2
    ] / jnp.maximum(added[3:4], 1.0)

    pl.when(s + 1 < count)(tail.wait_send)
    swap.wait_send()
    trade.wait_send()
    for i in range(1, count):
        target_copy(i).wait_send()
        token_copy(i).wait_send()
    own_main(False)
    own_mixed(False)
    for group in events:
        for event in group:
            event(False)
    for head in range(2):
        sent = gathered.at[head, pl.ds(0, devices - 1)]
        pltpu.make_async_copy(sent, sent, stat_send.at[head]).wait()


def fused(
    hidden,
    embedded,
    targets,
    main_mask,
    mtp_mask,
    lengths,
    head_weight,
    projection,
    main_gain,
    hidden_gain,
    embed_gain,
    mtp_gain,
):
    batches, seq_len, width = hidden.shape
    count, vocab = lax.axis_size("seq"), lax.axis_size("vocab")
    cols, feature = head_weight.shape[1], projection.shape[1]
    rows = batches * seq_len
    height = rows // 2
    split = height - height // SHARE
    memory = pl.BlockSpec(memory_space=pl.ANY)
    local = pl.BlockSpec(memory_space=pltpu.VMEM)
    scalar = pl.BlockSpec(memory_space=pltpu.SMEM)
    chunks = count * 5
    main_tokens, mtp_tokens, total_loss = pl.pallas_call(
        functools.partial(fused_kernel, (count // 2, split)),
        out_shape=[
            jax.ShapeDtypeStruct((2, height), jnp.float32),
            jax.ShapeDtypeStruct((2, height), jnp.float32),
            jax.ShapeDtypeStruct((1, 1), jnp.float32),
        ],
        in_specs=[memory] * 4 + [local] * 3 + [scalar] + [local] * 4,
        out_specs=[local] * 3,
        scratch_shapes=[
            pltpu.VMEM((2 * count, height, width), jnp.bfloat16),
            pltpu.VMEM((2 * cols, width), jnp.bfloat16),
            pltpu.VMEM((2 * width, feature), jnp.bfloat16),
            pltpu.VMEM((rows, width), jnp.bfloat16),
            pltpu.VMEM((rows, width), jnp.bfloat16),
            pltpu.VMEM((rows, 2 * width), jnp.bfloat16),
            pltpu.VMEM((rows, feature), jnp.bfloat16),
            pltpu.VMEM((batches, width), jnp.bfloat16),
            pltpu.VMEM((batches, width), jnp.bfloat16),
            pltpu.VMEM((count, 8, height), jnp.int32),
            pltpu.VMEM((height, width), jnp.bfloat16),
            pltpu.VMEM((height, 128), jnp.int32),
            pltpu.VMEM((height, 128), jnp.float32),
            pltpu.VMEM((height, 128), jnp.float32),
            pltpu.VMEM((height, 128), jnp.float32),
            pltpu.VMEM((2 * count, 8, height), jnp.float32),
            pltpu.VMEM((2, count * vocab, 8, height), jnp.float32),
            pltpu.VMEM((count, 8, height), jnp.float32),
            pltpu.SemaphoreType.DMA((5,)),
            pltpu.SemaphoreType.DMA((4, chunks)),
            pltpu.SemaphoreType.DMA((chunks,)),
            pltpu.SemaphoreType.DMA((3 + 2 * count,)),
            pltpu.SemaphoreType.DMA((3 + 2 * count,)),
            pltpu.SemaphoreType.DMA((2,)),
            pltpu.SemaphoreType.DMA((2,)),
        ],
        compiler_params=pltpu.CompilerParams(
            collective_id=0, has_side_effects=True, vmem_limit_bytes=60 * 2**20
        ),
    )(
        hidden.reshape(rows, width),
        embedded.reshape(rows, width),
        head_weight.T,
        projection,
        targets,
        main_mask,
        mtp_mask,
        lengths,
        main_gain.reshape(1, -1),
        hidden_gain.reshape(1, -1),
        embed_gain.reshape(1, -1),
        mtp_gain.reshape(1, -1),
    )
    return main_tokens, mtp_tokens, total_loss.reshape(())


def program(hidden, embedded, targets, *rest):
    one_tile = hidden.shape[0] == 2 and hidden.shape[1] == 128 and rest[4].shape[1] % 64 == 0
    if lax.axis_size("vocab") == 4 and one_tile:
        return fused(hidden, embedded, targets, *rest)
    return shards(hidden, embedded, targets, *rest)


def solution(mesh):
    return jax.shard_map(
        program,
        mesh=mesh,
        in_specs=(
            P(None, "seq", None),
            P(None, "seq", None),
            P(None, "seq"),
            P(None, "seq"),
            P(None, "seq"),
            P(),
            P(None, ("seq", "vocab")),
            P(None, "vocab"),
            P(),
            P(),
            P(),
            P(),
        ),
        out_specs=(P(None, "seq"), P(None, "seq"), P()),
        check_vma=False,
    )
```

```python
import functools
import heapq
import itertools

import jax
import jax.numpy as jnp
from jax import lax
from jax.experimental import pallas as pl
from jax.experimental.pallas import tpu as pltpu
from jax.sharding import PartitionSpec as P

EPSILON = 1e-06
MTP_WEIGHT = 0.3
CHUNK = 256
SHARE = 4
STEPS = 1
PIECES = 10
SWAPS = 5
MODEL_RATE, MODEL_DELAY, MODEL_START, MODEL_MIXED = 43.5e3, 2.0, 3.5, 10.0
MODEL_STEP, MODEL_NORM = 4.0, 0.7
ROWS = (((1,), (1,)), ((), ()))
MESH = pl.DeviceIdType.MESH


def from_behind(block, axis, distance):
    devices = range(lax.axis_size(axis))
    route = [(i - distance, i) for i in devices if i - distance in devices]
    return lax.ppermute(block, axis, route)


def normalize(values, gain_vec):
    values = values.astype(jnp.float32)
    mean_square = jnp.mean(values * values, axis=-1, keepdims=True)
    return values * lax.rsqrt(mean_square + EPSILON) * gain_vec


def join_stats(earlier, latter):
    highest = jnp.maximum(earlier[0], latter[0])
    exp_total = earlier[1] * jnp.exp(earlier[0] - highest) + latter[1] * jnp.exp(
        latter[0] - highest
    )
    return (highest, exp_total, earlier[2] + latter[2])


def seq_perm(value, bit):
    pairs = [(i, i ^ (1 << bit)) for i in range(lax.axis_size("seq"))]
    return lax.ppermute(value, "seq", pairs)


def vocab_perm(value, bit):
    pairs = [(i, i ^ (1 << bit)) for i in range(lax.axis_size("vocab"))]
    return lax.ppermute(value, "vocab", pairs)


def bits_of(axis):
    return list(reversed(range(lax.axis_size(axis).bit_length() - 1)))


def slot_masks(axis):
    masks = [0]
    for bit in bits_of(axis):
        masks = masks + [mask | (1 << bit) for mask in masks]
    return jnp.array(masks, jnp.int32)


def gather_pieces(own):
    pieces = [own]
    for bit in bits_of("seq"):
        held = pieces[0] if len(pieces) == 1 else jnp.concatenate(pieces, axis=0)
        pieces.append(seq_perm(held, bit))
    return pieces


def head_kernel(masks, at_ref, order_ref, *refs):
    blocks = refs[: len(masks)]
    gain_ref, local_ref, w_ref, out_ref, rows_ref = refs[len(masks) :]
    rows, width = rows_ref.shape
    part = blocks[0].shape[2]
    values = [block[0].astype(jnp.float32) for block in blocks]
    square = sum(jnp.sum(v * v, axis=1, keepdims=True) for v in values)
    scale = lax.rsqrt(square / width + EPSILON)
    for mask, value in zip(masks, values):
        place = pl.ds(pl.multiple_of((at_ref[0] ^ mask) * part, part), part)
        rows_ref[:, place] = (value * scale * gain_ref[:, place]).astype(jnp.bfloat16)
    wanted = local_ref[0]
    cols = w_ref.shape[1]
    stats = None
    for start in range(0, cols, CHUNK):
        stop = min(start + CHUNK, cols)
        logits = jnp.dot(
            rows_ref[...], w_ref[:, start:stop], preferred_element_type=jnp.float32
        )
        ids = lax.broadcasted_iota(jnp.int32, logits.shape, 1) + start
        highest = jnp.max(logits, axis=1, keepdims=True)
        total = jnp.sum(jnp.exp(logits - highest), axis=1, keepdims=True)
        picked = jnp.sum(jnp.where(ids == wanted, logits, 0.0), axis=1, keepdims=True)
        fresh = (highest, total, picked)
        stats = fresh if stats is None else join_stats(stats, fresh)
    lane = lax.broadcasted_iota(jnp.int32, (rows, 128), 1)
    packed = jnp.where(lane == 0, stats[0], jnp.where(lane == 1, stats[1], stats[2]))
    out_ref[0] = packed.T[:8]


def head_stats(masks, at, order, blocks, gain, local, head_weight):
    count, rows, part = blocks[0].shape
    width, cols = head_weight.shape
    flops = 2 * count * rows * width * cols
    return pl.pallas_call(
        functools.partial(head_kernel, masks),
        out_shape=jax.ShapeDtypeStruct((count, 8, rows), jnp.float32),
        grid_spec=pltpu.PrefetchScalarGridSpec(
            num_scalar_prefetch=2,
            grid=(count,),
            in_specs=[pl.BlockSpec((1, rows, part), lambda i, at, order: (i, 0, 0)) for _ in blocks]
            + [
                pl.BlockSpec((1, width), lambda i, at, order: (0, 0)),
                pl.BlockSpec((1, rows, 1), lambda i, at, order: (i, 0, 0)),
                pl.BlockSpec((width, cols), lambda i, at, order: (0, 0)),
            ],
            out_specs=pl.BlockSpec((1, 8, rows), lambda i, at, order: (order[i], 0, 0)),
            scratch_shapes=[pltpu.VMEM((rows, width), jnp.bfloat16)],
        ),
        compiler_params=pltpu.CompilerParams(vmem_limit_bytes=48 * 2**20),
        cost_estimate=pl.CostEstimate(
            flops=flops, bytes_accessed=2 * (width * cols + count * rows * width), transcendentals=count * rows * cols
        ),
    )(at, order, *blocks, gain.reshape(1, -1), local, head_weight)


def join_all(stats):
    highest = jnp.max(stats[:, 0], axis=0)
    total = jnp.sum(stats[:, 1] * jnp.exp(stats[:, 0] - highest), axis=0)
    return jnp.stack([highest, total, jnp.sum(stats[:, 2], axis=0)])


def finish(main_stats, mtp_stats):
    packed = jnp.concatenate([main_stats[:, :3], mtp_stats[:, :3]], axis=2)
    mine = lax.all_to_all(packed, "seq", 0, 0, tiled=True)
    joined = join_all(lax.all_gather(join_all(mine), "vocab"))
    return joined[0] + jnp.log(joined[1]) - joined[2]


def shards(
    hidden,
    embedded,
    targets,
    main_mask,
    mtp_mask,
    lengths,
    head_weight,
    projection,
    main_gain,
    hidden_gain,
    embed_gain,
    mtp_gain,
):
    batches, seq_len, model_width = hidden.shape
    rows = batches * seq_len
    seq_index = lax.axis_index("seq")
    vocab_index = lax.axis_index("vocab")
    vocab_count = lax.axis_size("vocab")
    cols = head_weight.shape[1]

    incoming = from_behind(hidden[:, seq_len - 1 :, :], "seq", 1)

    core = vocab_index & 1
    half = model_width // 2
    flat = hidden.reshape(1, rows, model_width)
    mine = lax.dynamic_slice_in_dim(flat, core * half, half, axis=2)
    other = lax.dynamic_slice_in_dim(flat, (1 - core) * half, half, axis=2)
    main_pieces = gather_pieces(mine)
    main_other = [other] + [vocab_perm(piece, 0) for piece in main_pieces[1:]]
    main_blocks = [jnp.concatenate(p, axis=0) for p in (main_pieces, main_other)]

    wanted = jnp.concatenate(gather_pieces(targets.reshape(1, rows)), axis=0)
    local = (wanted - (seq_index * vocab_count + vocab_index) * cols)[:, :, None]

    previous = jnp.concatenate([incoming, hidden[:, : seq_len - 1, :]], axis=1)
    joined = jnp.concatenate(
        [normalize(previous, hidden_gain), normalize(embedded, embed_gain)], axis=2
    )
    joined = joined.astype(jnp.bfloat16).reshape(rows, 2 * model_width)
    mixed = jnp.dot(joined, projection, preferred_element_type=jnp.float32).astype(jnp.bfloat16)
    masks = [0]
    held = [gather_pieces(mixed[None])]
    for bit in bits_of("vocab"):
        masks = masks + [mask | (1 << bit) for mask in masks]
        held = held + [[vocab_perm(piece, bit) for piece in pieces] for pieces in held]
    mtp_blocks = [jnp.concatenate(pieces, axis=0) for pieces in held]

    order = slot_masks("seq") ^ seq_index
    with jax.named_scope("mainhead"):
        main_stats = head_stats((0, 1), core[None], order, main_blocks, main_gain, local, head_weight)
    mtp_stats = head_stats(
        tuple(masks), vocab_index[None], order, mtp_blocks, mtp_gain, local, head_weight
    )

    positions = seq_index * seq_len + lax.broadcasted_iota(jnp.int32, (batches, seq_len), 1)
    inside = positions + 1 < lengths[:, None]
    keep_main = ((main_mask == 1) & inside).astype(jnp.float32)
    keep_mtp = ((mtp_mask == 1) & (positions >= 1) & inside).astype(jnp.float32)
    losses = finish(main_stats, mtp_stats).reshape(2, batches, seq_len)
    main_tokens = keep_main * losses[0]
    mtp_tokens = keep_mtp * losses[1]
    sums = jnp.stack(
        [jnp.sum(main_tokens), jnp.sum(mtp_tokens), jnp.sum(keep_main), jnp.sum(keep_mtp)]
    )
    for bit in bits_of("seq"):
        sums = sums + seq_perm(sums, bit)
    total_loss = sums[0] / jnp.maximum(sums[2], 1.0) + MTP_WEIGHT * sums[1] / jnp.maximum(
        sums[3], 1.0
    )
    return (main_tokens, mtp_tokens, total_loss)


def line_rank(place, count, j):
    near = jnp.minimum(place, count - 1 - place)
    lower = place < count - 1 - place
    step = (j + 1) // 2 * (2 * lax.rem(j, 2) - 1)
    close = jnp.where(lower, place + step, place - step)
    return jnp.where(j <= 2 * near, close, jnp.where(lower, j, count - 1 - j))


def rms_rows(values, gain, width):
    square = jnp.sum(values * values, axis=1, keepdims=True)
    return values * lax.rsqrt(square / width + EPSILON) * gain


def pick(table, index):
    value = table[0]
    for at, entry in enumerate(table[1:], 1):
        value = jnp.where(index == at, entry, value)
    return value


def onward(order, way, home=False):
    if way is None:
        ways, later = [], order
    else:
        axis = "z" if way in "+-" else way
        ways, later = ([way] if axis == "z" else []), order[order.index(axis) + 1 :]
    for axis in later:
        if axis == "z":
            ways += ["+", "-"]
        elif not (axis == "y" and home):
            ways.append(axis)
    return ways


def nearest(place, count, j):
    near = min(place, count - 1 - place)
    lower = place < count - 1 - place
    step = (j + 1) // 2 * (2 * (j % 2) - 1)
    if j <= 2 * near:
        return place + step if lower else place - step
    return j if lower else count - 1 - j


def plan(depth, pieces, steps):
    ticket = itertools.count()
    queue, free, waiting = [], {}, {}
    inbox, ready, pairs, served = ([[] for _ in range(depth)] for _ in range(4))
    parts = {head: set() for head in range(2)}
    for name, (head, _, order) in pieces.items():
        for of in range(2) if name == "b" else [head]:
            parts[of] |= {(name, part) for part in range(2 if "y" in order else 1)}
    held = [{} for _ in range(depth)]
    ranks = [{nearest(z, depth, j): j for j in range(depth)} for z in range(depth)]
    idle, taken = [MODEL_MIXED] * depth, [0] * depth

    def push(time, *what):
        heapq.heappush(queue, (time, next(ticket), what))

    def kick(z, way, time):
        line = waiting.get((z, way))
        if not line or free.get((z, way), 0) > time + 1e-9:
            return
        piece = line.pop(0)
        name, source, across, part = piece
        free[z, way] = time + pieces[name][1] / MODEL_RATE
        push(free[z, way], "free", z, way)
        if way == "x":
            piece = (name, source, 1 - across, part)
        elif way == "y":
            piece = (name, source, across, 1 - part)
        to = z + {"+": 1, "-": -1}.get(way, 0)
        push(free[z, way] + MODEL_DELAY, "arrive", to, piece, way)

    def send(z, piece, way, time):
        home = pieces[piece[0]][0] == 0 and piece[1:3] == (z, 0)
        for to in onward(pieces[piece[0]][2], way, home):
            if 0 <= z + {"+": 1, "-": -1}.get(to, 0) < depth:
                waiting.setdefault((z, to), []).append(piece)
                kick(z, to, time)

    def hold(z, piece):
        for head in range(2) if piece[0] == "b" else [pieces[piece[0]][0]]:
            block = (head, *piece[1:3])
            got = held[z].setdefault(block, set())
            got.add((piece[0], piece[3]))
            if block == (0, z, 0):
                got |= parts[0]
            if got == parts[head] and block not in ready[z]:
                ready[z].append(block)

    def turn(z, time):
        if idle[z] > time + 1e-9:
            return
        while inbox[z]:
            piece, way = inbox[z].pop(0)
            name, source, across, part = piece
            served[z].append((taken[z], name, ranks[z][source], across, part, way))
            send(z, piece, way, time)
        cost = MODEL_STEP
        if taken[z] == steps * len(pairs[z]):
            pair = ready[z][2 * len(pairs[z]) :][:2]
            if len(pair) < 2:
                return
            pairs[z].append([(head, ranks[z][source], across) for head, source, across in pair])
            cost += MODEL_NORM
        taken[z] += 1
        idle[z] = time + cost
        push(idle[z], "turn", z)

    for z in range(depth):
        push(MODEL_START, "own", z, 0)
        push(MODEL_MIXED, "own", z, 1)
    while queue:
        time, _, (what, z, *rest) = heapq.heappop(queue)
        if what == "free":
            kick(z, rest[0], time)
        elif what == "own":
            for name, (head, _, _) in pieces.items():
                if head == rest[0]:
                    hold(z, (name, z, 0, 0))
                    send(z, (name, z, 0, 0), None, time)
        elif what == "arrive":
            hold(z, rest[0])
            if onward(pieces[rest[0][0]][2], rest[1]):
                inbox[z].append(rest)
        turn(z, time)
    classes = (depth + 1) // 2
    return served[:classes], pairs[:classes]


def fused_kernel(
    sizes,
    hidden,
    embedded,
    weight,
    projection,
    targets,
    main_mask,
    mtp_mask,
    lengths,
    main_gain,
    hidden_gain,
    embed_gain,
    mtp_gain,
    result,
    grid,
    wide,
    proj,
    own_hidden,
    own_embedded,
    joined,
    mixed,
    last,
    behind,
    wanted,
    rows,
    want,
    highs,
    sums,
    picks,
    packed,
    gathered,
    tokens,
    load_sem,
    send_sem,
    recv_sem,
    small_send,
    small_recv,
    stat_send,
    stat_recv,
    swap_send,
    swap_recv,
):
    depth, spots, pieces = sizes
    count = depth * 2
    s, v = lax.axis_index("seq"), lax.axis_index("vocab")
    vocab = lax.axis_size("vocab")
    z, x, y, c = s // 2, s % 2, v // 2, v % 2
    height, width = rows.shape[0] // 2, rows.shape[1]
    half = width // 2
    feature = mixed.shape[1]
    cols = weight.shape[0]
    split = spots
    columns_of = pl.ds(pl.multiple_of(c * cols, 16), cols)

    def place(z_at, x_at, y_at, c_at):
        return (z_at * 2 + x_at, y_at * 2 + c_at)

    mine = pl.ds(pl.multiple_of(c * height, height), height)
    loads = [
        pltpu.make_async_copy(hidden.at[mine], grid.at[s], load_sem.at[0]),
        pltpu.make_async_copy(hidden, own_hidden, load_sem.at[1]),
        pltpu.make_async_copy(embedded, own_embedded, load_sem.at[2]),
        pltpu.make_async_copy(projection, proj, load_sem.at[3]),
        pltpu.make_async_copy(weight, wide.at[columns_of], load_sem.at[4]),
    ]
    for load in loads[:3]:
        load.start()

    barrier = pltpu.get_barrier_semaphore()
    devices = count * vocab
    ends_z = [(z + 1 < depth, place(z + 1, x, y, c)), (z > 0, place(z - 1, x, y, c))]
    cross = jnp.where(x == 1, z + 1, z - 1)
    ends_z.append(((cross >= 0) & (cross < depth), place(cross, 1 - x, y, c)))
    for other in (place(z, 1 - x, y, c), place(z, x, 1 - y, c), place(z, x, y, 1 - c)):
        pl.semaphore_signal(barrier, inc=1, device_id=other, device_id_type=MESH)
    greeted = 3
    for here, other in ends_z:

        @pl.when(here)
        def _(other=other):
            pl.semaphore_signal(barrier, inc=1, device_id=other, device_id_type=MESH)

        greeted = greeted + jnp.where(here, 1, 0)
    loads[3].start()
    loads[4].start()
    wanted[s] = jnp.broadcast_to(targets[pl.ds(c, 1), :], wanted.shape[1:])
    loads[1].wait()
    for b in range(2):
        last[b : b + 1, :] = own_hidden[(b + 1) * height - 1 : (b + 1) * height, :]
    pl.semaphore_wait(barrier, greeted)

    def chunk(kind, at, part):
        if kind == "b":
            return grid.at[at, pl.ds(split, height - split)], count * 2 + at
        if kind == "ids":
            return wanted.at[at], count * 5 + at
        columns = pl.ds(pl.multiple_of(part * half, half), half)
        if kind == "a":
            return grid.at[at, pl.ds(0, split), columns], at * 2 + part
        return grid.at[count + at, :, columns], count * 3 + at * 2 + part

    def send(go, kind, at, part, way, device, when=None):
        if kind == "b":
            send(go, "ids", at, part, way, device, when)
        ref, index = chunk(kind, at, part)
        copy = pltpu.make_async_remote_copy(
            src_ref=ref,
            dst_ref=ref,
            send_sem=send_sem.at[way, index],
            recv_sem=recv_sem.at[index],
            device_id=device,
            device_id_type=MESH,
        )
        act = copy.start if go else copy.wait_send
        if when is None:
            act()
        else:
            pl.when(when)(act)

    def arrive(go, kind, at, part):
        if not go:
            return
        if kind == "b":
            arrive(go, "ids", at, part)
        ref, index = chunk(kind, at, part)
        pltpu.make_async_remote_copy(
            src_ref=ref,
            dst_ref=ref,
            send_sem=send_sem.at[0, index],
            recv_sem=recv_sem.at[index],
            device_id=(s, v),
            device_id_type=MESH,
        ).wait_recv()

    def z_both(go, kind, at, part):
        send(go, kind, at, part, 0, place(z + 1, x, y, c), z + 1 < depth)
        send(go, kind, at, part, 1, place(z - 1, x, y, c), z > 0)

    def z_on(go, kind, at, part, origin):
        onward = jnp.where(origin < z, z + 1, z - 1)
        when = (onward >= 0) & (onward < depth)
        send(go, kind, at, part, 0, place(onward, x, y, c), when)

    def x_over(go, kind, at, part):
        send(go, kind, at, part, 2, place(z, 1 - x, y, c))

    def y_over(go, kind, at, part):
        send(go, kind, at, part, 3, place(z, x, 1 - y, c))

    def at_of(jz, jx):
        return line_rank(z, depth, jnp.int32(jz)) * 2 + lax.rem(x + jx, 2)

    def pass_on(go, kind, at, part, ways, origin=None):
        for way in ways:
            if way == "x":
                x_over(go, kind, at, part)
            elif way == "y":
                y_over(go, kind, at, part)
            elif origin is not None:
                z_on(go, kind, at, part, origin)
        if origin is None and "+" in ways:
            z_both(go, kind, at, part)

    def serve(go, kind, jz, jx, part, way):
        at = at_of(jz, jx)
        part = y if part == 0 else 1 - y
        arrive(go, kind, at, part)
        if way in "+-":
            later = [to for to in onward(pieces[kind][2], way) if to not in "+-"]
            z_on(go, kind, at, part, line_rank(z, depth, jnp.int32(jz)))
            pass_on(go, kind, at, part, later)
        else:
            pass_on(go, kind, at, part, onward(pieces[kind][2], way))

    def leaves(head, jz, jx, known):
        for kind, (of, _, order) in pieces.items():
            of = head if kind == "b" and not known else -1 if kind == "b" else of
            for part in range(2 if "y" in order else 1):
                moved = {"z": jz > 0, "x": jx > 0, "y": part > 0}
                ways = [axis for axis in order if moved[axis]]
                home = jz == 0 and jx == 0 and kind != "t"
                if of == head and ways and not home and ways[-1] == order[-1] and ways[-1] != "z":
                    arrive(True, kind, at_of(jz, jx), y if part == 0 else 1 - y)

    def own_main(go):
        for kind in ("a", "b"):
            pass_on(go, kind, s, y, onward(pieces[kind][2], None, True))

    def own_mixed(go):
        pass_on(go, "t", s, y, onward(pieces["t"][2], None))

    tail = pltpu.make_async_remote_copy(
        src_ref=last,
        dst_ref=behind,
        send_sem=small_send.at[0],
        recv_sem=small_recv.at[0],
        device_id=(s + 1, v),
        device_id_type=MESH,
    )
    pl.when(s + 1 < count)(tail.start)
    loads[0].wait()
    own_main(True)

    def swap(i):
        size = cols // SWAPS
        return pltpu.make_async_remote_copy(
            src_ref=weight.at[pl.ds(i * size, size)],
            dst_ref=wide.at[pl.ds(pl.multiple_of(c * cols + i * size, 16), size)],
            send_sem=swap_send.at[i],
            recv_sem=swap_recv.at[i],
            device_id=place(z, x, y, 1 - c),
            device_id_type=MESH,
        )

    for i in range(SWAPS // 2):
        swap(i).start()

    loads[2].wait()
    slab = 128

    def norm_inputs(i, carry):
        part = pl.ds(pl.multiple_of(i * slab, slab), slab)
        value = own_embedded[part, :].astype(jnp.float32)
        joined[part, width:] = rms_rows(value, embed_gain[...], width).astype(jnp.bfloat16)
        return carry

    lax.fori_loop(0, 2 * height // slab, norm_inputs, 0)
    def shifted(b, start, size, above):
        value = own_hidden[b * height + start : b * height + start + size, :].astype(jnp.float32)
        value = pltpu.roll(rms_rows(value, hidden_gain[...], width), 1, 0)
        row = lax.broadcasted_iota(jnp.int32, value.shape, 0)
        return jnp.where(row == 0, above, value).astype(jnp.bfloat16)

    for b in range(2):
        joined[b * height : (b + 1) * height, :width] = shifted(b, 0, height, 0.0)

    @pl.when(s == 0)
    def _():
        behind[...] = jnp.zeros_like(behind)

    @pl.when(s > 0)
    def _():
        tail.wait_recv()

    first = rms_rows(behind[...].astype(jnp.float32), hidden_gain[...], width)
    for b in range(2):
        joined[b * height : b * height + 16, :width] = shifted(b, 0, 16, first[b : b + 1, :])
    loads[3].wait()
    mixed[...] = jnp.dot(
        joined[...], proj[...], preferred_element_type=jnp.float32
    ).astype(jnp.bfloat16)
    place_of = pl.ds(pl.multiple_of(v * feature, feature), feature)
    other = pl.ds(pl.multiple_of((1 - c) * height, height), height)
    trade = pltpu.make_async_remote_copy(
        src_ref=mixed.at[other],
        dst_ref=grid.at[count + s, :, place_of],
        send_sem=small_send.at[2 + count],
        recv_sem=small_recv.at[2 + count],
        device_id=place(z, x, y, 1 - c),
        device_id_type=MESH,
    )
    trade.start()
    grid[count + s, :, place_of] = mixed[mine, :]
    trade.wait_recv()
    own_mixed(True)
    for i in range(SWAPS // 2, SWAPS):
        swap(i).start()
    loads[4].wait()

    served, pairs = plan(depth, pieces, STEPS)
    near = jnp.minimum(z, depth - 1 - z)

    def code_of(head, jz, jx):
        return head * count + jz * 2 + jx

    turns = range(len(pairs[0]))
    codes = [[[code_of(*pairs[k][i][side]) for k in range(len(pairs))] for i in turns] for side in range(2)]
    span = 2 * cols // STEPS
    piece_cols = span // PIECES

    def stat_copy(head, at, i):
        return pltpu.make_async_remote_copy(
            src_ref=packed.at[head * count + at],
            dst_ref=gathered.at[head, c * count * 2 + s * 2 + y],
            send_sem=stat_send.at[head],
            recv_sem=stat_recv.at[head],
            device_id=(at, lax.rem(v + i, vocab)),
            device_id_type=MESH,
        )

    def unit(step, carry):
        turn, sub = step // STEPS, lax.rem(step, STEPS)
        blocks = []
        for side in range(2):
            code = pick([pick(entry, near) for entry in codes[side]], turn)
            head, jz, jx = code // count, lax.rem(code, count) // 2, lax.rem(code, 2)
            blocks.append((head, line_rank(z, depth, jz) * 2 + lax.rem(x + jx, 2)))
        for k, events in enumerate(served):

            @pl.when(near == k)
            def _(k=k, events=events):
                for at_step in sorted({event[0] for event in events}):

                    @pl.when(step == at_step)
                    def _(at_step=at_step):
                        for when, *event in events:
                            if when == at_step:
                                serve(True, *event)

                @pl.when(sub == 0)
                def _():
                    for i, pair in enumerate(pairs[k]):

                        @pl.when(turn == i)
                        def _(pair=pair):
                            for block in pair:
                                before = [other for both in pairs[k] for other in both]
                                before = before[: before.index(block)]
                                leaves(*block, (1 - block[0], *block[1:]) in before)

        @pl.when(step == 0)
        def _():
            for i in range(SWAPS):
                swap(i).wait_recv()

        @pl.when(sub == 0)
        def _():
            for side, (head, at) in enumerate(blocks):
                gain = jnp.where(head == 0, main_gain[...], mtp_gain[...])

                def norm(i, carry, side=side, head=head, at=at, gain=gain):
                    part = pl.ds(pl.multiple_of(i * slab, slab), slab)
                    value = grid[head * count + at, part, :].astype(jnp.float32)
                    to = pl.ds(pl.multiple_of(side * height + i * slab, slab), slab)
                    rows[to, :] = rms_rows(value, gain, width).astype(jnp.bfloat16)
                    return carry

                lax.fori_loop(0, height // slab, norm, 0)
                want[:, side * height : (side + 1) * height] = wanted[at]
            highs[...] = jnp.full_like(highs, -1e30)
            sums[...] = jnp.zeros_like(sums)
            picks[...] = jnp.zeros_like(picks)

        begin = sub * span
        sublane = lax.broadcasted_iota(jnp.int32, want.shape, 0)
        relative = want[...] - sublane - (s * vocab + y * 2) * cols - begin
        high, total, picked = highs[...], sums[...], picks[...]
        for start in range(0, span, piece_cols):
            columns = pl.ds(pl.multiple_of(begin + start, 16), piece_cols)
            logits = lax.dot_general(
                wide[columns, :], rows[...], ROWS, preferred_element_type=jnp.float32
            )
            tiles = logits.reshape(piece_cols // 8, 8, 2 * height)
            higher = jnp.maximum(high, jnp.max(tiles, axis=0))
            total = total * jnp.exp(high - higher) + jnp.sum(jnp.exp(tiles - higher[None]), axis=0)
            ids = lax.broadcasted_iota(jnp.int32, tiles.shape, 0) * 8 + start
            picked = picked + jnp.sum(jnp.where(relative[None] == ids, tiles, 0.0), axis=0)
            high = higher
        highs[...], sums[...], picks[...] = high, total, picked

        @pl.when(sub == STEPS - 1)
        def _():
            top = jnp.max(high, axis=0, keepdims=True)
            added = jnp.sum(total * jnp.exp(high - top), axis=0, keepdims=True)
            found = jnp.sum(picked, axis=0, keepdims=True)
            block = jnp.where(sublane == 0, top, jnp.where(sublane == 1, added, found))
            for side, (head, at) in enumerate(blocks):
                packed[head * count + at] = block[:, side * height : (side + 1) * height]
            for head, at in blocks:
                for i in range(1, vocab):
                    stat_copy(head, at, i).start()

                @pl.when(at != s)
                def _(head=head, at=at):
                    stat_copy(head, at, 0).start()

                @pl.when(at == s)
                def _(head=head, at=at):
                    pltpu.make_async_copy(
                        packed.at[head * count + at],
                        gathered.at[head, c * count * 2 + s * 2 + y],
                        stat_recv.at[head],
                    ).start()

        return carry

    lax.fori_loop(0, STEPS * len(pairs[0]), unit, 0)

    pl.when(s + 1 < count)(tail.wait_send)
    for i in range(SWAPS):
        swap(i).wait_send()
    trade.wait_send()
    own_main(False)
    own_mixed(False)
    for k, events in enumerate(served):

        @pl.when(near == k)
        def _(events=events):
            for _, *event in events:
                serve(False, *event)

    for head in range(2):
        sent = gathered.at[head, pl.ds(0, devices - 1)]
        pltpu.make_async_copy(sent, sent, stat_send.at[head]).wait()

    lengths_of = [lengths[0], lengths[1]]
    position = s * height + lax.broadcasted_iota(jnp.int32, (1, height), 1)
    loss = [[None, None], [None, None]]
    group = count * 2
    for head in range(2):
        whole = gathered.at[head]
        pltpu.make_async_copy(whole, whole, stat_recv.at[head]).wait()
        for b in range(2):
            part = gathered[head, b * group : (b + 1) * group, 0:3, :]
            tops = part[:, 0, :]
            top = jnp.max(tops, axis=0, keepdims=True)
            added = jnp.sum(part[:, 1, :] * jnp.exp(tops - top), axis=0, keepdims=True)
            found = jnp.sum(part[:, 2, :], axis=0, keepdims=True)
            loss[head][b] = top + jnp.log(added) - found
    lines = [jnp.zeros((1, height), jnp.float32)] * 4
    for b in range(2):
        inside = position + 1 < lengths_of[b]
        keep = [
            jnp.where((main_mask[b : b + 1, :] == 1) & inside, 1.0, 0.0),
            jnp.where((mtp_mask[b : b + 1, :] == 1) & (position >= 1) & inside, 1.0, 0.0),
        ]
        for head in range(2):
            kept = keep[head] * loss[head][b]
            result[2 * head + b : 2 * head + b + 1, :] = kept
            lines[head] = lines[head] + kept
            lines[2 + head] = lines[2 + head] + keep[head]
    sub = lax.broadcasted_iota(jnp.int32, (8, height), 0)
    tile = jnp.zeros((8, height), jnp.float32)
    for at, line in enumerate(lines):
        tile = jnp.where(sub == at, line, tile)
    tokens[s] = tile

    def token_copy(i):
        return pltpu.make_async_remote_copy(
            src_ref=tokens.at[s],
            dst_ref=tokens.at[s],
            send_sem=small_send.at[3 + count + i],
            recv_sem=small_recv.at[3 + count + s],
            device_id=(lax.rem(s + i, count), v),
            device_id_type=MESH,
        )

    for i in range(1, count):
        token_copy(i).start()
    for i in range(1, count):
        source = lax.rem(s + i, count)
        pltpu.make_async_remote_copy(
            src_ref=tokens.at[source],
            dst_ref=tokens.at[source],
            send_sem=small_send.at[3 + count + i],
            recv_sem=small_recv.at[3 + count + source],
            device_id=(s, v),
            device_id_type=MESH,
        ).wait_recv()
    added = tokens[0]
    for i in range(1, count):
        added = added + tokens[i]
    added = jnp.sum(added, axis=1, keepdims=True)
    main_mean = added[0:1] / jnp.maximum(added[2:3], 1.0)
    mtp_mean = added[1:2] / jnp.maximum(added[3:4], 1.0)
    result[4:8, :] = jnp.broadcast_to(main_mean + MTP_WEIGHT * mtp_mean, (4, height))

    for i in range(1, count):
        token_copy(i).wait_send()


def fused(
    hidden,
    embedded,
    targets,
    main_mask,
    mtp_mask,
    lengths,
    head_weight,
    projection,
    main_gain,
    hidden_gain,
    embed_gain,
    mtp_gain,
):
    batches, seq_len, width = hidden.shape
    count, vocab = lax.axis_size("seq"), lax.axis_size("vocab")
    cols, feature = head_weight.shape[1], projection.shape[1]
    rows = batches * seq_len
    height = rows // 2
    split = height - height // SHARE
    pieces = {
        "a": (0, split * width, "xzy"),
        "b": (0, 2 * (height - split) * width, "zx"),
        "t": (1, height * width, "zyx"),
    }
    memory = pl.BlockSpec(memory_space=pl.ANY)
    local = pl.BlockSpec(memory_space=pltpu.VMEM)
    scalar = pl.BlockSpec(memory_space=pltpu.SMEM)
    chunks = count * 6
    result = pl.pallas_call(
        functools.partial(fused_kernel, (count // 2, split, pieces)),
        out_shape=jax.ShapeDtypeStruct((8, height), jnp.float32),
        in_specs=[memory] * 4 + [local] * 3 + [scalar] + [local] * 4,
        out_specs=local,
        scratch_shapes=[
            pltpu.VMEM((2 * count, height, width), jnp.bfloat16),
            pltpu.VMEM((2 * cols, width), jnp.bfloat16),
            pltpu.VMEM((2 * width, feature), jnp.bfloat16),
            pltpu.VMEM((rows, width), jnp.bfloat16),
            pltpu.VMEM((rows, width), jnp.bfloat16),
            pltpu.VMEM((rows, 2 * width), jnp.bfloat16),
            pltpu.VMEM((rows, feature), jnp.bfloat16),
            pltpu.VMEM((batches, width), jnp.bfloat16),
            pltpu.VMEM((batches, width), jnp.bfloat16),
            pltpu.VMEM((count, 8, height), jnp.int32),
            pltpu.VMEM((rows, width), jnp.bfloat16),
            pltpu.VMEM((8, rows), jnp.int32),
            pltpu.VMEM((8, rows), jnp.float32),
            pltpu.VMEM((8, rows), jnp.float32),
            pltpu.VMEM((8, rows), jnp.float32),
            pltpu.VMEM((2 * count, 8, height), jnp.float32),
            pltpu.VMEM((2, count * vocab, 8, height), jnp.float32),
            pltpu.VMEM((count, 8, height), jnp.float32),
            pltpu.SemaphoreType.DMA((5,)),
            pltpu.SemaphoreType.DMA((4, chunks)),
            pltpu.SemaphoreType.DMA((chunks,)),
            pltpu.SemaphoreType.DMA((3 + 2 * count,)),
            pltpu.SemaphoreType.DMA((3 + 2 * count,)),
            pltpu.SemaphoreType.DMA((2,)),
            pltpu.SemaphoreType.DMA((2,)),
            pltpu.SemaphoreType.DMA((SWAPS,)),
            pltpu.SemaphoreType.DMA((SWAPS,)),
        ],
        compiler_params=pltpu.CompilerParams(
            collective_id=0, has_side_effects=True, vmem_limit_bytes=60 * 2**20
        ),
    )(
        hidden.reshape(rows, width),
        embedded.reshape(rows, width),
        head_weight.T,
        projection,
        targets,
        main_mask,
        mtp_mask,
        lengths,
        main_gain.reshape(1, -1),
        hidden_gain.reshape(1, -1),
        embed_gain.reshape(1, -1),
        mtp_gain.reshape(1, -1),
    )
    return result[0:2], result[2:4], result[4, 0]


def program(hidden, embedded, targets, *rest):
    one_tile = hidden.shape[0] == 2 and hidden.shape[1] == 128 and rest[3].shape[1] % (8 * STEPS * PIECES) == 0
    if lax.axis_size("vocab") == 4 and one_tile:
        return fused(hidden, embedded, targets, *rest)
    return shards(hidden, embedded, targets, *rest)


def solution(mesh):
    return jax.shard_map(
        program,
        mesh=mesh,
        in_specs=(
            P(None, "seq", None),
            P(None, "seq", None),
            P(None, "seq"),
            P(None, "seq"),
            P(None, "seq"),
            P(),
            P(None, ("seq", "vocab")),
            P(None, "vocab"),
            P(),
            P(),
            P(),
            P(),
        ),
        out_specs=(P(None, "seq"), P(None, "seq"), P()),
        check_vma=False,
    )
```

```python
import functools
import heapq
import itertools

import jax
import jax.numpy as jnp
from jax import lax
from jax.experimental import pallas as pl
from jax.experimental.pallas import tpu as pltpu
from jax.sharding import PartitionSpec as P

EPSILON = 1e-06
MTP_WEIGHT = 0.3
CHUNK = 256
SHARE = 4
STEPS = 1
PIECES = 10
SWAPS = 5
MODEL_RATE, MODEL_DELAY, MODEL_START, MODEL_MIXED = 45e3, 2.5, 3.3, 8.5
MODEL_STEP, MODEL_NORM = 4.1, 0.5
ROWS = (((1,), (1,)), ((), ()))
MESH = pl.DeviceIdType.MESH
KINDS = ("a", "b", "ids", "t")


def from_behind(block, axis, distance):
    devices = range(lax.axis_size(axis))
    route = [(i - distance, i) for i in devices if i - distance in devices]
    return lax.ppermute(block, axis, route)


def normalize(values, gain_vec):
    values = values.astype(jnp.float32)
    mean_square = jnp.mean(values * values, axis=-1, keepdims=True)
    return values * lax.rsqrt(mean_square + EPSILON) * gain_vec


def join_stats(earlier, latter):
    highest = jnp.maximum(earlier[0], latter[0])
    exp_total = earlier[1] * jnp.exp(earlier[0] - highest) + latter[1] * jnp.exp(
        latter[0] - highest
    )
    return (highest, exp_total, earlier[2] + latter[2])


def seq_perm(value, bit):
    pairs = [(i, i ^ (1 << bit)) for i in range(lax.axis_size("seq"))]
    return lax.ppermute(value, "seq", pairs)


def vocab_perm(value, bit):
    pairs = [(i, i ^ (1 << bit)) for i in range(lax.axis_size("vocab"))]
    return lax.ppermute(value, "vocab", pairs)


def bits_of(axis):
    return list(reversed(range(lax.axis_size(axis).bit_length() - 1)))


def slot_masks(axis):
    masks = [0]
    for bit in bits_of(axis):
        masks = masks + [mask | (1 << bit) for mask in masks]
    return jnp.array(masks, jnp.int32)


def gather_pieces(own):
    pieces = [own]
    for bit in bits_of("seq"):
        held = pieces[0] if len(pieces) == 1 else jnp.concatenate(pieces, axis=0)
        pieces.append(seq_perm(held, bit))
    return pieces


def head_kernel(masks, at_ref, order_ref, *refs):
    blocks = refs[: len(masks)]
    gain_ref, local_ref, w_ref, out_ref, rows_ref = refs[len(masks) :]
    rows, width = rows_ref.shape
    part = blocks[0].shape[2]
    values = [block[0].astype(jnp.float32) for block in blocks]
    square = sum(jnp.sum(v * v, axis=1, keepdims=True) for v in values)
    scale = lax.rsqrt(square / width + EPSILON)
    for mask, value in zip(masks, values):
        place = pl.ds(pl.multiple_of((at_ref[0] ^ mask) * part, part), part)
        rows_ref[:, place] = (value * scale * gain_ref[:, place]).astype(jnp.bfloat16)
    wanted = local_ref[0]
    cols = w_ref.shape[1]
    stats = None
    for start in range(0, cols, CHUNK):
        stop = min(start + CHUNK, cols)
        logits = jnp.dot(
            rows_ref[...], w_ref[:, start:stop], preferred_element_type=jnp.float32
        )
        ids = lax.broadcasted_iota(jnp.int32, logits.shape, 1) + start
        highest = jnp.max(logits, axis=1, keepdims=True)
        total = jnp.sum(jnp.exp(logits - highest), axis=1, keepdims=True)
        picked = jnp.sum(jnp.where(ids == wanted, logits, 0.0), axis=1, keepdims=True)
        fresh = (highest, total, picked)
        stats = fresh if stats is None else join_stats(stats, fresh)
    lane = lax.broadcasted_iota(jnp.int32, (rows, 128), 1)
    packed = jnp.where(lane == 0, stats[0], jnp.where(lane == 1, stats[1], stats[2]))
    out_ref[0] = packed.T[:8]


def head_stats(masks, at, order, blocks, gain, local, head_weight):
    count, rows, part = blocks[0].shape
    width, cols = head_weight.shape
    flops = 2 * count * rows * width * cols
    return pl.pallas_call(
        functools.partial(head_kernel, masks),
        out_shape=jax.ShapeDtypeStruct((count, 8, rows), jnp.float32),
        grid_spec=pltpu.PrefetchScalarGridSpec(
            num_scalar_prefetch=2,
            grid=(count,),
            in_specs=[pl.BlockSpec((1, rows, part), lambda i, at, order: (i, 0, 0)) for _ in blocks]
            + [
                pl.BlockSpec((1, width), lambda i, at, order: (0, 0)),
                pl.BlockSpec((1, rows, 1), lambda i, at, order: (i, 0, 0)),
                pl.BlockSpec((width, cols), lambda i, at, order: (0, 0)),
            ],
            out_specs=pl.BlockSpec((1, 8, rows), lambda i, at, order: (order[i], 0, 0)),
            scratch_shapes=[pltpu.VMEM((rows, width), jnp.bfloat16)],
        ),
        compiler_params=pltpu.CompilerParams(vmem_limit_bytes=48 * 2**20),
        cost_estimate=pl.CostEstimate(
            flops=flops, bytes_accessed=2 * (width * cols + count * rows * width), transcendentals=count * rows * cols
        ),
    )(at, order, *blocks, gain.reshape(1, -1), local, head_weight)


def join_all(stats):
    highest = jnp.max(stats[:, 0], axis=0)
    total = jnp.sum(stats[:, 1] * jnp.exp(stats[:, 0] - highest), axis=0)
    return jnp.stack([highest, total, jnp.sum(stats[:, 2], axis=0)])


def finish(main_stats, mtp_stats):
    packed = jnp.concatenate([main_stats[:, :3], mtp_stats[:, :3]], axis=2)
    mine = lax.all_to_all(packed, "seq", 0, 0, tiled=True)
    joined = join_all(lax.all_gather(join_all(mine), "vocab"))
    return joined[0] + jnp.log(joined[1]) - joined[2]


def shards(
    hidden,
    embedded,
    targets,
    main_mask,
    mtp_mask,
    lengths,
    head_weight,
    projection,
    main_gain,
    hidden_gain,
    embed_gain,
    mtp_gain,
):
    batches, seq_len, model_width = hidden.shape
    rows = batches * seq_len
    seq_index = lax.axis_index("seq")
    vocab_index = lax.axis_index("vocab")
    vocab_count = lax.axis_size("vocab")
    cols = head_weight.shape[1]

    incoming = from_behind(hidden[:, seq_len - 1 :, :], "seq", 1)

    core = vocab_index & 1
    half = model_width // 2
    flat = hidden.reshape(1, rows, model_width)
    mine = lax.dynamic_slice_in_dim(flat, core * half, half, axis=2)
    other = lax.dynamic_slice_in_dim(flat, (1 - core) * half, half, axis=2)
    main_pieces = gather_pieces(mine)
    main_other = [other] + [vocab_perm(piece, 0) for piece in main_pieces[1:]]
    main_blocks = [jnp.concatenate(p, axis=0) for p in (main_pieces, main_other)]

    wanted = jnp.concatenate(gather_pieces(targets.reshape(1, rows)), axis=0)
    local = (wanted - (seq_index * vocab_count + vocab_index) * cols)[:, :, None]

    previous = jnp.concatenate([incoming, hidden[:, : seq_len - 1, :]], axis=1)
    joined = jnp.concatenate(
        [normalize(previous, hidden_gain), normalize(embedded, embed_gain)], axis=2
    )
    joined = joined.astype(jnp.bfloat16).reshape(rows, 2 * model_width)
    mixed = jnp.dot(joined, projection, preferred_element_type=jnp.float32).astype(jnp.bfloat16)
    masks = [0]
    held = [gather_pieces(mixed[None])]
    for bit in bits_of("vocab"):
        masks = masks + [mask | (1 << bit) for mask in masks]
        held = held + [[vocab_perm(piece, bit) for piece in pieces] for pieces in held]
    mtp_blocks = [jnp.concatenate(pieces, axis=0) for pieces in held]

    order = slot_masks("seq") ^ seq_index
    with jax.named_scope("mainhead"):
        main_stats = head_stats((0, 1), core[None], order, main_blocks, main_gain, local, head_weight)
    mtp_stats = head_stats(
        tuple(masks), vocab_index[None], order, mtp_blocks, mtp_gain, local, head_weight
    )

    positions = seq_index * seq_len + lax.broadcasted_iota(jnp.int32, (batches, seq_len), 1)
    inside = positions + 1 < lengths[:, None]
    keep_main = ((main_mask == 1) & inside).astype(jnp.float32)
    keep_mtp = ((mtp_mask == 1) & (positions >= 1) & inside).astype(jnp.float32)
    losses = finish(main_stats, mtp_stats).reshape(2, batches, seq_len)
    main_tokens = keep_main * losses[0]
    mtp_tokens = keep_mtp * losses[1]
    sums = jnp.stack(
        [jnp.sum(main_tokens), jnp.sum(mtp_tokens), jnp.sum(keep_main), jnp.sum(keep_mtp)]
    )
    for bit in bits_of("seq"):
        sums = sums + seq_perm(sums, bit)
    total_loss = sums[0] / jnp.maximum(sums[2], 1.0) + MTP_WEIGHT * sums[1] / jnp.maximum(
        sums[3], 1.0
    )
    return (main_tokens, mtp_tokens, total_loss)


def line_rank(place, count, j):
    near = jnp.minimum(place, count - 1 - place)
    lower = place < count - 1 - place
    step = (j + 1) // 2 * (2 * lax.rem(j, 2) - 1)
    close = jnp.where(lower, place + step, place - step)
    return jnp.where(j <= 2 * near, close, jnp.where(lower, j, count - 1 - j))


def rms_rows(values, gain, width):
    square = jnp.sum(values * values, axis=1, keepdims=True)
    return values * lax.rsqrt(square / width + EPSILON) * gain


def pick(table, index):
    value = table[0]
    for at, entry in enumerate(table[1:], 1):
        value = jnp.where(index == at, entry, value)
    return value


def onward(order, way, home=False):
    if way is None:
        ways, later = [], order
    else:
        axis = "z" if way in "+-" else way
        ways, later = ([way] if axis == "z" else []), order[order.index(axis) + 1 :]
    for axis in later:
        if axis == "z":
            ways += ["+", "-"]
        elif not (axis == "y" and home):
            ways.append(axis)
    return ways


def nearest(place, count, j):
    near = min(place, count - 1 - place)
    lower = place < count - 1 - place
    step = (j + 1) // 2 * (2 * (j % 2) - 1)
    if j <= 2 * near:
        return place + step if lower else place - step
    return j if lower else count - 1 - j


def plan(depth, pieces, steps):
    ticket = itertools.count()
    queue, free, waiting = [], {}, {}
    inbox, ready, pairs, served = ([[] for _ in range(depth)] for _ in range(4))
    parts = {head: set() for head in range(2)}
    for name, (head, _, order) in pieces.items():
        for of in range(2) if name == "b" else [head]:
            parts[of] |= {(name, part) for part in range(2 if "y" in order else 1)}
    held = [{} for _ in range(depth)]
    ranks = [{nearest(z, depth, j): j for j in range(depth)} for z in range(depth)]
    idle, taken = [MODEL_MIXED] * depth, [0] * depth

    def push(time, *what):
        heapq.heappush(queue, (time, next(ticket), what))

    def kick(z, way, time):
        line = waiting.get((z, way))
        if not line or free.get((z, way), 0) > time + 1e-9:
            return
        piece = line.pop(0)
        name, source, across, part = piece
        free[z, way] = time + pieces[name][1] / MODEL_RATE
        push(free[z, way], "free", z, way)
        if way == "x":
            piece = (name, source, 1 - across, part)
        elif way == "y":
            piece = (name, source, across, 1 - part)
        to = z + {"+": 1, "-": -1}.get(way, 0)
        push(free[z, way] + MODEL_DELAY, "arrive", to, piece, way)

    def send(z, piece, way, time):
        home = pieces[piece[0]][0] == 0 and piece[1:3] == (z, 0)
        for to in onward(pieces[piece[0]][2], way, home):
            if 0 <= z + {"+": 1, "-": -1}.get(to, 0) < depth:
                waiting.setdefault((z, to), []).append(piece)
                kick(z, to, time)

    def hold(z, piece):
        for head in range(2) if piece[0] == "b" else [pieces[piece[0]][0]]:
            block = (head, *piece[1:3])
            got = held[z].setdefault(block, set())
            got.add((piece[0], piece[3]))
            if block == (0, z, 0):
                got |= parts[0]
            if got == parts[head] and block not in ready[z]:
                ready[z].append(block)

    def turn(z, time):
        if idle[z] > time + 1e-9:
            return
        while inbox[z]:
            piece, way = inbox[z].pop(0)
            name, source, across, part = piece
            served[z].append((taken[z], name, ranks[z][source], across, part, way))
            send(z, piece, way, time)
        cost = MODEL_STEP
        if taken[z] == steps * len(pairs[z]):
            pair = ready[z][2 * len(pairs[z]) :][:2]
            if len(pair) < 2:
                return
            pairs[z].append([(head, ranks[z][source], across) for head, source, across in pair])
            cost += MODEL_NORM
        taken[z] += 1
        idle[z] = time + cost
        push(idle[z], "turn", z)

    for z in range(depth):
        push(MODEL_START, "own", z, 0)
        push(MODEL_MIXED, "own", z, 1)
    while queue:
        time, _, (what, z, *rest) = heapq.heappop(queue)
        if what == "free":
            kick(z, rest[0], time)
        elif what == "own":
            for name, (head, _, _) in pieces.items():
                if head == rest[0]:
                    hold(z, (name, z, 0, 0))
                    send(z, (name, z, 0, 0), None, time)
        elif what == "arrive":
            hold(z, rest[0])
            if onward(pieces[rest[0][0]][2], rest[1]):
                inbox[z].append(rest)
        turn(z, time)
    classes = (depth + 1) // 2
    return served[:classes], pairs[:classes]


def fused_kernel(
    sizes,
    hidden,
    embedded,
    weight,
    projection,
    targets,
    main_mask,
    mtp_mask,
    lengths,
    main_gain,
    hidden_gain,
    embed_gain,
    mtp_gain,
    result,
    grid,
    wide,
    proj,
    own_hidden,
    own_embedded,
    joined,
    mixed,
    last,
    behind,
    wanted,
    rows,
    want,
    highs,
    sums,
    picks,
    packed,
    gathered,
    tokens,
    load_sem,
    send_sem,
    recv_sem,
    small_send,
    small_recv,
    stat_send,
    stat_recv,
    swap_send,
    swap_recv,
):
    depth, spots, pieces = sizes
    count = depth * 2
    s, v = lax.axis_index("seq"), lax.axis_index("vocab")
    vocab = lax.axis_size("vocab")
    z, x, y, c = s // 2, s % 2, v // 2, v % 2
    height, width = rows.shape[0] // 2, rows.shape[1]
    half = width // 2
    feature = mixed.shape[1]
    cols = weight.shape[0]
    split = spots
    columns_of = pl.ds(pl.multiple_of(c * cols, 16), cols)

    def place(z_at, x_at, y_at, c_at):
        return (z_at * 2 + x_at, y_at * 2 + c_at)

    mine = pl.ds(pl.multiple_of(c * height, height), height)
    loads = [
        pltpu.make_async_copy(hidden.at[mine], grid.at[s], load_sem.at[0]),
        pltpu.make_async_copy(hidden, own_hidden, load_sem.at[1]),
        pltpu.make_async_copy(embedded, own_embedded, load_sem.at[2]),
        pltpu.make_async_copy(projection, proj, load_sem.at[3]),
        pltpu.make_async_copy(weight, wide.at[columns_of], load_sem.at[4]),
    ]
    for load in (loads[1], loads[0], loads[2]):
        load.start()

    barrier = pltpu.get_barrier_semaphore()
    devices = count * vocab
    ends_z = [(z + 1 < depth, place(z + 1, x, y, c)), (z > 0, place(z - 1, x, y, c))]
    cross = jnp.where(x == 1, z + 1, z - 1)
    ends_z.append(((cross >= 0) & (cross < depth), place(cross, 1 - x, y, c)))
    for other in (place(z, 1 - x, y, c), place(z, x, 1 - y, c), place(z, x, y, 1 - c)):
        pl.semaphore_signal(barrier, inc=1, device_id=other, device_id_type=MESH)
    greeted = 3
    for here, other in ends_z:

        @pl.when(here)
        def _(other=other):
            pl.semaphore_signal(barrier, inc=1, device_id=other, device_id_type=MESH)

        greeted = greeted + jnp.where(here, 1, 0)
    loads[3].start()
    loads[4].start()
    wanted[s] = jnp.broadcast_to(targets[pl.ds(c, 1), :], wanted.shape[1:])
    loads[0].wait()
    pl.semaphore_wait(barrier, greeted)

    def chunk(kind, at, part):
        if kind == "b":
            return grid.at[at, pl.ds(split, height - split)], count * 2 + at
        if kind == "ids":
            return wanted.at[at], count * 5 + at
        columns = pl.ds(pl.multiple_of(part * half, half), half)
        if kind == "a":
            return grid.at[at, pl.ds(0, split), columns], at * 2 + part
        return grid.at[count + at, :, columns], count * 3 + at * 2 + part

    def send(kind, at, part, way, device, when=None):
        if kind == "b":
            send("ids", at, part, way, device, when)
        ref, index = chunk(kind, at, part)
        copy = pltpu.make_async_remote_copy(
            src_ref=ref,
            dst_ref=ref,
            send_sem=send_sem.at[KINDS.index(kind), way],
            recv_sem=recv_sem.at[index],
            device_id=device,
            device_id_type=MESH,
        )
        if when is None:
            copy.start()
        else:
            pl.when(when)(copy.start)

    def sent(kind, way, number):
        some = pl.ds(0, number)
        if kind == "a":
            ref = grid.at[some, pl.ds(0, split), pl.ds(0, half)]
        elif kind == "b":
            ref = grid.at[some, pl.ds(split, height - split)]
        elif kind == "t":
            ref = grid.at[some, :, pl.ds(0, half)]
        else:
            ref = wanted.at[some]
        pltpu.make_async_copy(ref, ref, send_sem.at[KINDS.index(kind), way]).wait()

    def arrive(kind, at, part):
        if kind == "b":
            arrive("ids", at, part)
        ref, index = chunk(kind, at, part)
        pltpu.make_async_remote_copy(
            src_ref=ref,
            dst_ref=ref,
            send_sem=send_sem.at[KINDS.index(kind), 0],
            recv_sem=recv_sem.at[index],
            device_id=(s, v),
            device_id_type=MESH,
        ).wait_recv()

    def z_both(kind, at, part):
        send(kind, at, part, 0, place(z + 1, x, y, c), z + 1 < depth)
        send(kind, at, part, 1, place(z - 1, x, y, c), z > 0)

    def z_on(kind, at, part, origin):
        onward = jnp.where(origin < z, z + 1, z - 1)
        when = (onward >= 0) & (onward < depth)
        send(kind, at, part, jnp.where(origin < z, 0, 1), place(onward, x, y, c), when)

    def x_over(kind, at, part):
        send(kind, at, part, 2, place(z, 1 - x, y, c))

    def y_over(kind, at, part):
        send(kind, at, part, 3, place(z, x, 1 - y, c))

    def at_of(jz, jx):
        return line_rank(z, depth, jnp.int32(jz)) * 2 + lax.rem(x + jx, 2)

    def pass_on(kind, at, part, ways, origin=None):
        for way in ways:
            if way == "x":
                x_over(kind, at, part)
            elif way == "y":
                y_over(kind, at, part)
            elif origin is not None:
                z_on(kind, at, part, origin)
        if origin is None and "+" in ways:
            z_both(kind, at, part)

    def serve(kind, jz, jx, part, way):
        at = at_of(jz, jx)
        part = y if part == 0 else 1 - y
        arrive(kind, at, part)
        if way in "+-":
            later = [to for to in onward(pieces[kind][2], way) if to not in "+-"]
            z_on(kind, at, part, line_rank(z, depth, jnp.int32(jz)))
            pass_on(kind, at, part, later)
        else:
            pass_on(kind, at, part, onward(pieces[kind][2], way))

    def leaves(head, jz, jx, known):
        for kind, (of, _, order) in pieces.items():
            of = head if kind == "b" and not known else -1 if kind == "b" else of
            for part in range(2 if "y" in order else 1):
                moved = {"z": jz > 0, "x": jx > 0, "y": part > 0}
                ways = [axis for axis in order if moved[axis]]
                home = jz == 0 and jx == 0 and kind != "t"
                if of == head and ways and not home and ways[-1] == order[-1] and ways[-1] != "z":
                    arrive(kind, at_of(jz, jx), y if part == 0 else 1 - y)

    def own_main():
        for kind in ("a", "b"):
            pass_on(kind, s, y, onward(pieces[kind][2], None, True))

    def own_mixed():
        pass_on("t", s, y, onward(pieces["t"][2], None))

    loads[1].wait()
    for b in range(2):
        last[b : b + 1, :] = own_hidden[(b + 1) * height - 1 : (b + 1) * height, :]
    tail = pltpu.make_async_remote_copy(
        src_ref=last,
        dst_ref=behind,
        send_sem=small_send.at[0],
        recv_sem=small_recv.at[0],
        device_id=(s + 1, v),
        device_id_type=MESH,
    )
    pl.when(s + 1 < count)(tail.start)
    own_main()

    def swap(i):
        size = cols // SWAPS
        return pltpu.make_async_remote_copy(
            src_ref=weight.at[pl.ds(i * size, size)],
            dst_ref=wide.at[pl.ds(pl.multiple_of(c * cols + i * size, 16), size)],
            send_sem=swap_send.at[i],
            recv_sem=swap_recv.at[i],
            device_id=place(z, x, y, 1 - c),
            device_id_type=MESH,
        )


    loads[2].wait()
    slab = 128

    def norm_inputs(i, carry):
        part = pl.ds(pl.multiple_of(i * slab, slab), slab)
        value = own_embedded[part, :].astype(jnp.float32)
        joined[part, width:] = rms_rows(value, embed_gain[...], width).astype(jnp.bfloat16)
        return carry

    lax.fori_loop(0, 2 * height // slab, norm_inputs, 0)
    def shifted(b, start, size, above):
        value = own_hidden[b * height + start : b * height + start + size, :].astype(jnp.float32)
        value = pltpu.roll(rms_rows(value, hidden_gain[...], width), 1, 0)
        row = lax.broadcasted_iota(jnp.int32, value.shape, 0)
        return jnp.where(row == 0, above, value).astype(jnp.bfloat16)

    for b in range(2):
        joined[b * height : (b + 1) * height, :width] = shifted(b, 0, height, 0.0)

    @pl.when(s == 0)
    def _():
        behind[...] = jnp.zeros_like(behind)

    @pl.when(s > 0)
    def _():
        tail.wait_recv()

    first = rms_rows(behind[...].astype(jnp.float32), hidden_gain[...], width)
    for b in range(2):
        joined[b * height : b * height + 16, :width] = shifted(b, 0, 16, first[b : b + 1, :])
    loads[3].wait()
    mixed[...] = jnp.dot(
        joined[...], proj[...], preferred_element_type=jnp.float32
    ).astype(jnp.bfloat16)
    place_of = pl.ds(pl.multiple_of(v * feature, feature), feature)
    other = pl.ds(pl.multiple_of((1 - c) * height, height), height)
    trade = pltpu.make_async_remote_copy(
        src_ref=mixed.at[other],
        dst_ref=grid.at[count + s, :, place_of],
        send_sem=small_send.at[1],
        recv_sem=small_recv.at[1],
        device_id=place(z, x, y, 1 - c),
        device_id_type=MESH,
    )
    trade.start()
    grid[count + s, :, place_of] = mixed[mine, :]
    trade.wait_recv()
    own_mixed()
    for i in range(SWAPS):
        swap(i).start()
    loads[4].wait()

    served, pairs = plan(depth, pieces, STEPS)
    near = jnp.minimum(z, depth - 1 - z)

    def code_of(head, jz, jx):
        return head * count + jz * 2 + jx

    turns = range(len(pairs[0]))
    codes = [[[code_of(*pairs[k][i][side]) for k in range(len(pairs))] for i in turns] for side in range(2)]
    span = 2 * cols // STEPS
    piece_cols = span // PIECES

    def stat_copy(head, at, i):
        return pltpu.make_async_remote_copy(
            src_ref=packed.at[head * count + at],
            dst_ref=gathered.at[head, c * count * 2 + s * 2 + y],
            send_sem=stat_send.at[head],
            recv_sem=stat_recv.at[head],
            device_id=(at, lax.rem(v + i, vocab)),
            device_id_type=MESH,
        )

    def unit(step, carry):
        turn, sub = step // STEPS, lax.rem(step, STEPS)
        blocks = []
        for side in range(2):
            code = pick([pick(entry, near) for entry in codes[side]], turn)
            head, jz, jx = code // count, lax.rem(code, count) // 2, lax.rem(code, 2)
            blocks.append((head, line_rank(z, depth, jz) * 2 + lax.rem(x + jx, 2)))
        for k, events in enumerate(served):

            @pl.when(near == k)
            def _(k=k, events=events):
                for at_step in sorted({event[0] for event in events}):

                    @pl.when(step == at_step)
                    def _(at_step=at_step):
                        for when, *event in events:
                            if when == at_step:
                                serve(*event)

                @pl.when(sub == 0)
                def _():
                    for i, pair in enumerate(pairs[k]):

                        @pl.when(turn == i)
                        def _(pair=pair):
                            for block in pair:
                                before = [other for both in pairs[k] for other in both]
                                before = before[: before.index(block)]
                                leaves(*block, (1 - block[0], *block[1:]) in before)

        @pl.when(step == 0)
        def _():
            for i in range(SWAPS):
                swap(i).wait_recv()

        @pl.when(sub == 0)
        def _():
            for side, (head, at) in enumerate(blocks):
                gain = jnp.where(head == 0, main_gain[...], mtp_gain[...])

                def norm(i, carry, side=side, head=head, at=at, gain=gain):
                    part = pl.ds(pl.multiple_of(i * slab, slab), slab)
                    value = grid[head * count + at, part, :].astype(jnp.float32)
                    to = pl.ds(pl.multiple_of(side * height + i * slab, slab), slab)
                    rows[to, :] = rms_rows(value, gain, width).astype(jnp.bfloat16)
                    return carry

                lax.fori_loop(0, height // slab, norm, 0)
                want[:, side * height : (side + 1) * height] = wanted[at]
            highs[...] = jnp.full_like(highs, -1e30)
            sums[...] = jnp.zeros_like(sums)
            picks[...] = jnp.zeros_like(picks)

        begin = sub * span
        sublane = lax.broadcasted_iota(jnp.int32, want.shape, 0)
        relative = want[...] - sublane - (s * vocab + y * 2) * cols - begin
        high, total, picked = highs[...], sums[...], picks[...]
        for start in range(0, span, piece_cols):
            columns = pl.ds(pl.multiple_of(begin + start, 16), piece_cols)
            logits = lax.dot_general(
                wide[columns, :], rows[...], ROWS, preferred_element_type=jnp.float32
            )
            tiles = logits.reshape(piece_cols // 8, 8, 2 * height)
            higher = jnp.maximum(high, jnp.max(tiles, axis=0))
            total = total * jnp.exp(high - higher) + jnp.sum(jnp.exp(tiles - higher[None]), axis=0)
            ids = lax.broadcasted_iota(jnp.int32, tiles.shape, 0) * 8 + start
            picked = picked + jnp.sum(jnp.where(relative[None] == ids, tiles, 0.0), axis=0)
            high = higher
        highs[...], sums[...], picks[...] = high, total, picked

        @pl.when(sub == STEPS - 1)
        def _():
            top = jnp.max(high, axis=0, keepdims=True)
            added = jnp.sum(total * jnp.exp(high - top), axis=0, keepdims=True)
            found = jnp.sum(picked, axis=0, keepdims=True)
            block = jnp.where(sublane == 0, top, jnp.where(sublane == 1, added, found))
            for side, (head, at) in enumerate(blocks):
                packed[head * count + at] = block[:, side * height : (side + 1) * height]
            for head, at in blocks:
                for i in range(1, vocab):
                    stat_copy(head, at, i).start()

                @pl.when(at != s)
                def _(head=head, at=at):
                    stat_copy(head, at, 0).start()

                @pl.when(at == s)
                def _(head=head, at=at):
                    pltpu.make_async_copy(
                        packed.at[head * count + at],
                        gathered.at[head, c * count * 2 + s * 2 + y],
                        stat_recv.at[head],
                    ).start()

        return carry

    lax.fori_loop(0, STEPS * len(pairs[0]), unit, 0)

    pl.when(s + 1 < count)(tail.wait_send)
    for i in range(SWAPS):
        swap(i).wait_send()
    trade.wait_send()
    for kind, over_x, over_y, on_z in (
        ("a", 1, count - 1, 2),
        ("b", depth, 0, 1),
        ("ids", depth, 0, 1),
        ("t", 2 * depth, depth, 1),
    ):
        sent(kind, 2, over_x)
        if over_y:
            sent(kind, 3, over_y)
        for k in range(depth):

            @pl.when(z == k)
            def _(k=k, kind=kind, on_z=on_z):
                if k + 1 < depth:
                    sent(kind, 0, on_z * (k + 1))
                if k > 0:
                    sent(kind, 1, on_z * (depth - k))

    for head in range(2):
        others = gathered.at[head, pl.ds(0, devices - 1)]
        pltpu.make_async_copy(others, others, stat_send.at[head]).wait()

    lengths_of = [lengths[0], lengths[1]]
    position = s * height + lax.broadcasted_iota(jnp.int32, (1, height), 1)
    loss = [[None, None], [None, None]]
    group = count * 2
    for head in range(2):
        whole = gathered.at[head]
        pltpu.make_async_copy(whole, whole, stat_recv.at[head]).wait()
        for b in range(2):
            part = gathered[head, b * group : (b + 1) * group, 0:3, :]
            tops = part[:, 0, :]
            top = jnp.max(tops, axis=0, keepdims=True)
            added = jnp.sum(part[:, 1, :] * jnp.exp(tops - top), axis=0, keepdims=True)
            found = jnp.sum(part[:, 2, :], axis=0, keepdims=True)
            loss[head][b] = top + jnp.log(added) - found
    lines = [jnp.zeros((1, height), jnp.float32)] * 4
    for b in range(2):
        inside = position + 1 < lengths_of[b]
        keep = [
            jnp.where((main_mask[b : b + 1, :] == 1) & inside, 1.0, 0.0),
            jnp.where((mtp_mask[b : b + 1, :] == 1) & (position >= 1) & inside, 1.0, 0.0),
        ]
        for head in range(2):
            kept = keep[head] * loss[head][b]
            result[2 * head + b : 2 * head + b + 1, :] = kept
            lines[head] = lines[head] + kept
            lines[2 + head] = lines[2 + head] + keep[head]
    sub = lax.broadcasted_iota(jnp.int32, (8, height), 0)
    tile = jnp.zeros((8, height), jnp.float32)
    for at, line in enumerate(lines):
        tile = jnp.where(sub == at, line, tile)
    tokens[s] = tile

    def token_copy(i):
        return pltpu.make_async_remote_copy(
            src_ref=tokens.at[s],
            dst_ref=tokens.at[s],
            send_sem=small_send.at[2],
            recv_sem=small_recv.at[2],
            device_id=(lax.rem(s + i, count), v),
            device_id_type=MESH,
        )

    for i in range(1, count):
        token_copy(i).start()
    others = tokens.at[pl.ds(0, count - 1)]
    pltpu.make_async_copy(others, others, small_recv.at[2]).wait()
    added = tokens[0]
    for i in range(1, count):
        added = added + tokens[i]
    added = jnp.sum(added, axis=1, keepdims=True)
    main_mean = added[0:1] / jnp.maximum(added[2:3], 1.0)
    mtp_mean = added[1:2] / jnp.maximum(added[3:4], 1.0)
    spot = lax.broadcasted_iota(jnp.int32, (4, height), 0) + lax.broadcasted_iota(jnp.int32, (4, height), 1)
    result[4:8, :] = jnp.where(spot == 0, main_mean + MTP_WEIGHT * mtp_mean, 0.0)

    pltpu.make_async_copy(others, others, small_send.at[2]).wait()


def fused(
    hidden,
    embedded,
    targets,
    main_mask,
    mtp_mask,
    lengths,
    head_weight,
    projection,
    main_gain,
    hidden_gain,
    embed_gain,
    mtp_gain,
):
    batches, seq_len, width = hidden.shape
    count, vocab = lax.axis_size("seq"), lax.axis_size("vocab")
    cols, feature = head_weight.shape[1], projection.shape[1]
    rows = batches * seq_len
    height = rows // 2
    split = height - height // SHARE
    pieces = {
        "a": (0, split * width, "xzy"),
        "b": (0, 2 * (height - split) * width, "zx"),
        "t": (1, height * width, "zyx"),
    }
    memory = pl.BlockSpec(memory_space=pl.ANY)
    local = pl.BlockSpec(memory_space=pltpu.VMEM)
    scalar = pl.BlockSpec(memory_space=pltpu.SMEM)
    chunks = count * 6
    result = pl.pallas_call(
        functools.partial(fused_kernel, (count // 2, split, pieces)),
        out_shape=jax.ShapeDtypeStruct((8, height), jnp.float32),
        in_specs=[memory] * 4 + [local] * 3 + [scalar] + [local] * 4,
        out_specs=local,
        scratch_shapes=[
            pltpu.VMEM((2 * count, height, width), jnp.bfloat16),
            pltpu.VMEM((2 * cols, width), jnp.bfloat16),
            pltpu.VMEM((2 * width, feature), jnp.bfloat16),
            pltpu.VMEM((rows, width), jnp.bfloat16),
            pltpu.VMEM((rows, width), jnp.bfloat16),
            pltpu.VMEM((rows, 2 * width), jnp.bfloat16),
            pltpu.VMEM((rows, feature), jnp.bfloat16),
            pltpu.VMEM((batches, width), jnp.bfloat16),
            pltpu.VMEM((batches, width), jnp.bfloat16),
            pltpu.VMEM((count, 8, height), jnp.int32),
            pltpu.VMEM((rows, width), jnp.bfloat16),
            pltpu.VMEM((8, rows), jnp.int32),
            pltpu.VMEM((8, rows), jnp.float32),
            pltpu.VMEM((8, rows), jnp.float32),
            pltpu.VMEM((8, rows), jnp.float32),
            pltpu.VMEM((2 * count, 8, height), jnp.float32),
            pltpu.VMEM((2, count * vocab, 8, height), jnp.float32),
            pltpu.VMEM((count, 8, height), jnp.float32),
            pltpu.SemaphoreType.DMA((5,)),
            pltpu.SemaphoreType.DMA((len(KINDS), 4)),
            pltpu.SemaphoreType.DMA((chunks,)),
            pltpu.SemaphoreType.DMA((3,)),
            pltpu.SemaphoreType.DMA((3,)),
            pltpu.SemaphoreType.DMA((2,)),
            pltpu.SemaphoreType.DMA((2,)),
            pltpu.SemaphoreType.DMA((SWAPS,)),
            pltpu.SemaphoreType.DMA((SWAPS,)),
        ],
        compiler_params=pltpu.CompilerParams(
            collective_id=0, has_side_effects=True, vmem_limit_bytes=60 * 2**20
        ),
    )(
        hidden.reshape(rows, width),
        embedded.reshape(rows, width),
        head_weight.T,
        projection,
        targets,
        main_mask,
        mtp_mask,
        lengths,
        main_gain.reshape(1, -1),
        hidden_gain.reshape(1, -1),
        embed_gain.reshape(1, -1),
        mtp_gain.reshape(1, -1),
    )
    return result[0:2], result[2:4], jnp.sum(result[4:6])


def program(hidden, embedded, targets, *rest):
    one_tile = hidden.shape[0] == 2 and hidden.shape[1] == 128 and rest[3].shape[1] % (8 * STEPS * PIECES) == 0
    if lax.axis_size("vocab") == 4 and one_tile:
        return fused(hidden, embedded, targets, *rest)
    return shards(hidden, embedded, targets, *rest)


def solution(mesh):
    return jax.shard_map(
        program,
        mesh=mesh,
        in_specs=(
            P(None, "seq", None),
            P(None, "seq", None),
            P(None, "seq"),
            P(None, "seq"),
            P(None, "seq"),
            P(),
            P(None, ("seq", "vocab")),
            P(None, "vocab"),
            P(),
            P(),
            P(),
            P(),
        ),
        out_specs=(P(None, "seq"), P(None, "seq"), P()),
        check_vma=False,
    )
```

```python
import functools
import heapq
import itertools

import jax
import jax.numpy as jnp
from jax import lax
from jax.experimental import pallas as pl
from jax.experimental.pallas import tpu as pltpu
from jax.sharding import PartitionSpec as P

EPSILON = 1e-06
MTP_WEIGHT = 0.3
CHUNK = 256
SHARE = 4
STEPS = 1
PIECES = 8
SWAPS = 5
MODEL_RATE, MODEL_DELAY, MODEL_START, MODEL_MIXED = 45e3, 2.5, 3.3, 8.5
MODEL_STEP, MODEL_NORM = 4.1, 0.5
ROWS = (((1,), (1,)), ((), ()))
MESH = pl.DeviceIdType.MESH
KINDS = ("a", "b", "ids", "t")


def from_behind(block, axis, distance):
    devices = range(lax.axis_size(axis))
    route = [(i - distance, i) for i in devices if i - distance in devices]
    return lax.ppermute(block, axis, route)


def normalize(values, gain_vec):
    values = values.astype(jnp.float32)
    mean_square = jnp.mean(values * values, axis=-1, keepdims=True)
    return values * lax.rsqrt(mean_square + EPSILON) * gain_vec


def join_stats(earlier, latter):
    highest = jnp.maximum(earlier[0], latter[0])
    exp_total = earlier[1] * jnp.exp(earlier[0] - highest) + latter[1] * jnp.exp(
        latter[0] - highest
    )
    return (highest, exp_total, earlier[2] + latter[2])


def seq_perm(value, bit):
    pairs = [(i, i ^ (1 << bit)) for i in range(lax.axis_size("seq"))]
    return lax.ppermute(value, "seq", pairs)


def vocab_perm(value, bit):
    pairs = [(i, i ^ (1 << bit)) for i in range(lax.axis_size("vocab"))]
    return lax.ppermute(value, "vocab", pairs)


def bits_of(axis):
    return list(reversed(range(lax.axis_size(axis).bit_length() - 1)))


def slot_masks(axis):
    masks = [0]
    for bit in bits_of(axis):
        masks = masks + [mask | (1 << bit) for mask in masks]
    return jnp.array(masks, jnp.int32)


def gather_pieces(own):
    pieces = [own]
    for bit in bits_of("seq"):
        held = pieces[0] if len(pieces) == 1 else jnp.concatenate(pieces, axis=0)
        pieces.append(seq_perm(held, bit))
    return pieces


def head_kernel(masks, at_ref, order_ref, *refs):
    blocks = refs[: len(masks)]
    gain_ref, local_ref, w_ref, out_ref, rows_ref = refs[len(masks) :]
    rows, width = rows_ref.shape
    part = blocks[0].shape[2]
    values = [block[0].astype(jnp.float32) for block in blocks]
    square = sum(jnp.sum(v * v, axis=1, keepdims=True) for v in values)
    scale = lax.rsqrt(square / width + EPSILON)
    for mask, value in zip(masks, values):
        place = pl.ds(pl.multiple_of((at_ref[0] ^ mask) * part, part), part)
        rows_ref[:, place] = (value * scale * gain_ref[:, place]).astype(jnp.bfloat16)
    wanted = local_ref[0]
    cols = w_ref.shape[1]
    stats = None
    for start in range(0, cols, CHUNK):
        stop = min(start + CHUNK, cols)
        logits = jnp.dot(
            rows_ref[...], w_ref[:, start:stop], preferred_element_type=jnp.float32
        )
        ids = lax.broadcasted_iota(jnp.int32, logits.shape, 1) + start
        highest = jnp.max(logits, axis=1, keepdims=True)
        total = jnp.sum(jnp.exp(logits - highest), axis=1, keepdims=True)
        picked = jnp.sum(jnp.where(ids == wanted, logits, 0.0), axis=1, keepdims=True)
        fresh = (highest, total, picked)
        stats = fresh if stats is None else join_stats(stats, fresh)
    lane = lax.broadcasted_iota(jnp.int32, (rows, 128), 1)
    packed = jnp.where(lane == 0, stats[0], jnp.where(lane == 1, stats[1], stats[2]))
    out_ref[0] = packed.T[:8]


def head_stats(masks, at, order, blocks, gain, local, head_weight):
    count, rows, part = blocks[0].shape
    width, cols = head_weight.shape
    flops = 2 * count * rows * width * cols
    return pl.pallas_call(
        functools.partial(head_kernel, masks),
        out_shape=jax.ShapeDtypeStruct((count, 8, rows), jnp.float32),
        grid_spec=pltpu.PrefetchScalarGridSpec(
            num_scalar_prefetch=2,
            grid=(count,),
            in_specs=[pl.BlockSpec((1, rows, part), lambda i, at, order: (i, 0, 0)) for _ in blocks]
            + [
                pl.BlockSpec((1, width), lambda i, at, order: (0, 0)),
                pl.BlockSpec((1, rows, 1), lambda i, at, order: (i, 0, 0)),
                pl.BlockSpec((width, cols), lambda i, at, order: (0, 0)),
            ],
            out_specs=pl.BlockSpec((1, 8, rows), lambda i, at, order: (order[i], 0, 0)),
            scratch_shapes=[pltpu.VMEM((rows, width), jnp.bfloat16)],
        ),
        compiler_params=pltpu.CompilerParams(vmem_limit_bytes=48 * 2**20),
        cost_estimate=pl.CostEstimate(
            flops=flops, bytes_accessed=2 * (width * cols + count * rows * width), transcendentals=count * rows * cols
        ),
    )(at, order, *blocks, gain.reshape(1, -1), local, head_weight)


def join_all(stats):
    highest = jnp.max(stats[:, 0], axis=0)
    total = jnp.sum(stats[:, 1] * jnp.exp(stats[:, 0] - highest), axis=0)
    return jnp.stack([highest, total, jnp.sum(stats[:, 2], axis=0)])


def finish(main_stats, mtp_stats):
    packed = jnp.concatenate([main_stats[:, :3], mtp_stats[:, :3]], axis=2)
    mine = lax.all_to_all(packed, "seq", 0, 0, tiled=True)
    joined = join_all(lax.all_gather(join_all(mine), "vocab"))
    return joined[0] + jnp.log(joined[1]) - joined[2]


def shards(
    hidden,
    embedded,
    targets,
    main_mask,
    mtp_mask,
    lengths,
    head_weight,
    projection,
    main_gain,
    hidden_gain,
    embed_gain,
    mtp_gain,
):
    batches, seq_len, model_width = hidden.shape
    rows = batches * seq_len
    seq_index = lax.axis_index("seq")
    vocab_index = lax.axis_index("vocab")
    vocab_count = lax.axis_size("vocab")
    cols = head_weight.shape[1]

    incoming = from_behind(hidden[:, seq_len - 1 :, :], "seq", 1)

    core = vocab_index & 1
    half = model_width // 2
    flat = hidden.reshape(1, rows, model_width)
    mine = lax.dynamic_slice_in_dim(flat, core * half, half, axis=2)
    other = lax.dynamic_slice_in_dim(flat, (1 - core) * half, half, axis=2)
    main_pieces = gather_pieces(mine)
    main_other = [other] + [vocab_perm(piece, 0) for piece in main_pieces[1:]]
    main_blocks = [jnp.concatenate(p, axis=0) for p in (main_pieces, main_other)]

    wanted = jnp.concatenate(gather_pieces(targets.reshape(1, rows)), axis=0)
    local = (wanted - (seq_index * vocab_count + vocab_index) * cols)[:, :, None]

    previous = jnp.concatenate([incoming, hidden[:, : seq_len - 1, :]], axis=1)
    joined = jnp.concatenate(
        [normalize(previous, hidden_gain), normalize(embedded, embed_gain)], axis=2
    )
    joined = joined.astype(jnp.bfloat16).reshape(rows, 2 * model_width)
    mixed = jnp.dot(joined, projection, preferred_element_type=jnp.float32).astype(jnp.bfloat16)
    masks = [0]
    held = [gather_pieces(mixed[None])]
    for bit in bits_of("vocab"):
        masks = masks + [mask | (1 << bit) for mask in masks]
        held = held + [[vocab_perm(piece, bit) for piece in pieces] for pieces in held]
    mtp_blocks = [jnp.concatenate(pieces, axis=0) for pieces in held]

    order = slot_masks("seq") ^ seq_index
    with jax.named_scope("mainhead"):
        main_stats = head_stats((0, 1), core[None], order, main_blocks, main_gain, local, head_weight)
    mtp_stats = head_stats(
        tuple(masks), vocab_index[None], order, mtp_blocks, mtp_gain, local, head_weight
    )

    positions = seq_index * seq_len + lax.broadcasted_iota(jnp.int32, (batches, seq_len), 1)
    inside = positions + 1 < lengths[:, None]
    keep_main = ((main_mask == 1) & inside).astype(jnp.float32)
    keep_mtp = ((mtp_mask == 1) & (positions >= 1) & inside).astype(jnp.float32)
    losses = finish(main_stats, mtp_stats).reshape(2, batches, seq_len)
    main_tokens = keep_main * losses[0]
    mtp_tokens = keep_mtp * losses[1]
    sums = jnp.stack(
        [jnp.sum(main_tokens), jnp.sum(mtp_tokens), jnp.sum(keep_main), jnp.sum(keep_mtp)]
    )
    for bit in bits_of("seq"):
        sums = sums + seq_perm(sums, bit)
    total_loss = sums[0] / jnp.maximum(sums[2], 1.0) + MTP_WEIGHT * sums[1] / jnp.maximum(
        sums[3], 1.0
    )
    return (main_tokens, mtp_tokens, total_loss)


def line_rank(place, count, j):
    near = jnp.minimum(place, count - 1 - place)
    lower = place < count - 1 - place
    step = (j + 1) // 2 * (2 * lax.rem(j, 2) - 1)
    close = jnp.where(lower, place + step, place - step)
    return jnp.where(j <= 2 * near, close, jnp.where(lower, j, count - 1 - j))


def rms_rows(values, gain, width):
    square = jnp.sum(values * values, axis=1, keepdims=True)
    return values * lax.rsqrt(square / width + EPSILON) * gain


def pick(table, index):
    value = table[0]
    for at, entry in enumerate(table[1:], 1):
        value = jnp.where(index == at, entry, value)
    return value


def onward(order, way, home=False):
    if way is None:
        ways, later = [], order
    else:
        axis = "z" if way in "+-" else way
        ways, later = ([way] if axis == "z" else []), order[order.index(axis) + 1 :]
    for axis in later:
        if axis == "z":
            ways += ["+", "-"]
        elif not (axis == "y" and home):
            ways.append(axis)
    return ways


def nearest(place, count, j):
    near = min(place, count - 1 - place)
    lower = place < count - 1 - place
    step = (j + 1) // 2 * (2 * (j % 2) - 1)
    if j <= 2 * near:
        return place + step if lower else place - step
    return j if lower else count - 1 - j


def plan(depth, pieces, steps):
    ticket = itertools.count()
    queue, free, waiting = [], {}, {}
    inbox, ready, pairs, served = ([[] for _ in range(depth)] for _ in range(4))
    parts = {head: set() for head in range(2)}
    for name, (head, _, order) in pieces.items():
        for of in range(2) if name == "b" else [head]:
            parts[of] |= {(name, part) for part in range(2 if "y" in order else 1)}
    held = [{} for _ in range(depth)]
    ranks = [{nearest(z, depth, j): j for j in range(depth)} for z in range(depth)]
    idle, taken = [MODEL_MIXED] * depth, [0] * depth

    def push(time, *what):
        heapq.heappush(queue, (time, next(ticket), what))

    def kick(z, way, time):
        line = waiting.get((z, way))
        if not line or free.get((z, way), 0) > time + 1e-9:
            return
        piece = line.pop(0)
        name, source, across, part = piece
        free[z, way] = time + pieces[name][1] / MODEL_RATE
        push(free[z, way], "free", z, way)
        if way == "x":
            piece = (name, source, 1 - across, part)
        elif way == "y":
            piece = (name, source, across, 1 - part)
        to = z + {"+": 1, "-": -1}.get(way, 0)
        push(free[z, way] + MODEL_DELAY, "arrive", to, piece, way)

    def send(z, piece, way, time):
        home = pieces[piece[0]][0] == 0 and piece[1:3] == (z, 0)
        for to in onward(pieces[piece[0]][2], way, home):
            if 0 <= z + {"+": 1, "-": -1}.get(to, 0) < depth:
                waiting.setdefault((z, to), []).append(piece)
                kick(z, to, time)

    def hold(z, piece):
        for head in range(2) if piece[0] == "b" else [pieces[piece[0]][0]]:
            block = (head, *piece[1:3])
            got = held[z].setdefault(block, set())
            got.add((piece[0], piece[3]))
            if block == (0, z, 0):
                got |= parts[0]
            if got == parts[head] and block not in ready[z]:
                ready[z].append(block)

    def turn(z, time):
        if idle[z] > time + 1e-9:
            return
        while inbox[z]:
            piece, way = inbox[z].pop(0)
            name, source, across, part = piece
            served[z].append((taken[z], name, ranks[z][source], across, part, way))
            send(z, piece, way, time)
        cost = MODEL_STEP
        if taken[z] == steps * len(pairs[z]):
            pair = ready[z][2 * len(pairs[z]) :][:2]
            if len(pair) < 2:
                return
            pairs[z].append([(head, ranks[z][source], across) for head, source, across in pair])
            cost += MODEL_NORM
        taken[z] += 1
        idle[z] = time + cost
        push(idle[z], "turn", z)

    for z in range(depth):
        push(MODEL_START, "own", z, 0)
        push(MODEL_MIXED, "own", z, 1)
    while queue:
        time, _, (what, z, *rest) = heapq.heappop(queue)
        if what == "free":
            kick(z, rest[0], time)
        elif what == "own":
            for name, (head, _, _) in pieces.items():
                if head == rest[0]:
                    hold(z, (name, z, 0, 0))
                    send(z, (name, z, 0, 0), None, time)
        elif what == "arrive":
            hold(z, rest[0])
            if onward(pieces[rest[0][0]][2], rest[1]):
                inbox[z].append(rest)
        turn(z, time)
    classes = (depth + 1) // 2
    return served[:classes], pairs[:classes]


def fused_kernel(
    sizes,
    hidden,
    embedded,
    weight,
    projection,
    targets,
    main_mask,
    mtp_mask,
    lengths,
    main_gain,
    hidden_gain,
    embed_gain,
    mtp_gain,
    result,
    grid,
    wide,
    proj,
    own_hidden,
    own_embedded,
    joined,
    mixed,
    last,
    behind,
    wanted,
    rows,
    want,
    highs,
    sums,
    picks,
    packed,
    gathered,
    tokens,
    load_sem,
    send_sem,
    recv_sem,
    small_send,
    small_recv,
    stat_send,
    stat_recv,
    swap_send,
    swap_recv,
):
    depth, spots, pieces = sizes
    count = depth * 2
    s, v = lax.axis_index("seq"), lax.axis_index("vocab")
    vocab = lax.axis_size("vocab")
    z, x, y, c = s // 2, s % 2, v // 2, v % 2
    height, width = rows.shape[0] // 2, rows.shape[1]
    half = width // 2
    feature = mixed.shape[1]
    cols = weight.shape[0]
    split = spots
    columns_of = pl.ds(pl.multiple_of(c * cols, 16), cols)

    def place(z_at, x_at, y_at, c_at):
        return (z_at * 2 + x_at, y_at * 2 + c_at)

    mine = pl.ds(pl.multiple_of(c * height, height), height)
    loads = [
        pltpu.make_async_copy(hidden.at[mine], grid.at[s], load_sem.at[0]),
        pltpu.make_async_copy(hidden, own_hidden, load_sem.at[1]),
        pltpu.make_async_copy(embedded, own_embedded, load_sem.at[2]),
        pltpu.make_async_copy(projection, proj, load_sem.at[3]),
        pltpu.make_async_copy(weight, wide.at[columns_of], load_sem.at[4]),
    ]
    for load in (loads[1], loads[0], loads[2]):
        load.start()

    barrier = pltpu.get_barrier_semaphore()
    devices = count * vocab
    ends_z = [(z + 1 < depth, place(z + 1, x, y, c)), (z > 0, place(z - 1, x, y, c))]
    cross = jnp.where(x == 1, z + 1, z - 1)
    ends_z.append(((cross >= 0) & (cross < depth), place(cross, 1 - x, y, c)))
    for other in (place(z, 1 - x, y, c), place(z, x, 1 - y, c), place(z, x, y, 1 - c)):
        pl.semaphore_signal(barrier, inc=1, device_id=other, device_id_type=MESH)
    greeted = 3
    for here, other in ends_z:

        @pl.when(here)
        def _(other=other):
            pl.semaphore_signal(barrier, inc=1, device_id=other, device_id_type=MESH)

        greeted = greeted + jnp.where(here, 1, 0)
    loads[3].start()
    loads[4].start()
    wanted[s] = jnp.broadcast_to(targets[pl.ds(c, 1), :], wanted.shape[1:])
    loads[0].wait()
    pl.semaphore_wait(barrier, greeted)

    def chunk(kind, at, part):
        if kind == "b":
            return grid.at[at, pl.ds(split, height - split)], count * 2 + at
        if kind == "ids":
            return wanted.at[at], count * 5 + at
        columns = pl.ds(pl.multiple_of(part * half, half), half)
        if kind == "a":
            return grid.at[at, pl.ds(0, split), columns], at * 2 + part
        return grid.at[count + at, :, columns], count * 3 + at * 2 + part

    def send(kind, at, part, way, device, when=None):
        if kind == "b":
            send("ids", at, part, way, device, when)
        ref, index = chunk(kind, at, part)
        copy = pltpu.make_async_remote_copy(
            src_ref=ref,
            dst_ref=ref,
            send_sem=send_sem.at[KINDS.index(kind), way],
            recv_sem=recv_sem.at[index],
            device_id=device,
            device_id_type=MESH,
        )
        if when is None:
            copy.start()
        else:
            pl.when(when)(copy.start)

    def sent(kind, way, number):
        some = pl.ds(0, number)
        if kind == "a":
            ref = grid.at[some, pl.ds(0, split), pl.ds(0, half)]
        elif kind == "b":
            ref = grid.at[some, pl.ds(split, height - split)]
        elif kind == "t":
            ref = grid.at[some, :, pl.ds(0, half)]
        else:
            ref = wanted.at[some]
        pltpu.make_async_copy(ref, ref, send_sem.at[KINDS.index(kind), way]).wait()

    def arrive(kind, at, part):
        if kind == "b":
            arrive("ids", at, part)
        ref, index = chunk(kind, at, part)
        pltpu.make_async_remote_copy(
            src_ref=ref,
            dst_ref=ref,
            send_sem=send_sem.at[KINDS.index(kind), 0],
            recv_sem=recv_sem.at[index],
            device_id=(s, v),
            device_id_type=MESH,
        ).wait_recv()

    def z_both(kind, at, part):
        send(kind, at, part, 0, place(z + 1, x, y, c), z + 1 < depth)
        send(kind, at, part, 1, place(z - 1, x, y, c), z > 0)

    def z_on(kind, at, part, origin):
        onward = jnp.where(origin < z, z + 1, z - 1)
        when = (onward >= 0) & (onward < depth)
        send(kind, at, part, jnp.where(origin < z, 0, 1), place(onward, x, y, c), when)

    def x_over(kind, at, part):
        send(kind, at, part, 2, place(z, 1 - x, y, c))

    def y_over(kind, at, part):
        send(kind, at, part, 3, place(z, x, 1 - y, c))

    def at_of(jz, jx):
        return line_rank(z, depth, jnp.int32(jz)) * 2 + lax.rem(x + jx, 2)

    def pass_on(kind, at, part, ways, origin=None):
        for way in ways:
            if way == "x":
                x_over(kind, at, part)
            elif way == "y":
                y_over(kind, at, part)
            elif origin is not None:
                z_on(kind, at, part, origin)
        if origin is None and "+" in ways:
            z_both(kind, at, part)

    def serve(kind, jz, jx, part, way):
        at = at_of(jz, jx)
        part = y if part == 0 else 1 - y
        arrive(kind, at, part)
        if way in "+-":
            later = [to for to in onward(pieces[kind][2], way) if to not in "+-"]
            z_on(kind, at, part, line_rank(z, depth, jnp.int32(jz)))
            pass_on(kind, at, part, later)
        else:
            pass_on(kind, at, part, onward(pieces[kind][2], way))

    def leaves(head, jz, jx, known):
        for kind, (of, _, order) in pieces.items():
            of = head if kind == "b" and not known else -1 if kind == "b" else of
            for part in range(2 if "y" in order else 1):
                moved = {"z": jz > 0, "x": jx > 0, "y": part > 0}
                ways = [axis for axis in order if moved[axis]]
                home = jz == 0 and jx == 0 and kind != "t"
                if of == head and ways and not home and ways[-1] == order[-1] and ways[-1] != "z":
                    arrive(kind, at_of(jz, jx), y if part == 0 else 1 - y)

    def own_main():
        for kind in ("a", "b"):
            pass_on(kind, s, y, onward(pieces[kind][2], None, True))

    def own_mixed():
        pass_on("t", s, y, onward(pieces["t"][2], None))

    loads[1].wait()
    for b in range(2):
        last[b : b + 1, :] = own_hidden[(b + 1) * height - 1 : (b + 1) * height, :]
    tail = pltpu.make_async_remote_copy(
        src_ref=last,
        dst_ref=behind,
        send_sem=small_send.at[0],
        recv_sem=small_recv.at[0],
        device_id=(s + 1, v),
        device_id_type=MESH,
    )
    pl.when(s + 1 < count)(tail.start)
    own_main()

    def swap(i):
        size = cols // SWAPS
        return pltpu.make_async_remote_copy(
            src_ref=weight.at[pl.ds(i * size, size)],
            dst_ref=wide.at[pl.ds(pl.multiple_of(c * cols + i * size, 16), size)],
            send_sem=swap_send.at[i],
            recv_sem=swap_recv.at[i],
            device_id=place(z, x, y, 1 - c),
            device_id_type=MESH,
        )


    loads[2].wait()
    slab = 128

    def norm_inputs(i, carry):
        part = pl.ds(pl.multiple_of(i * slab, slab), slab)
        value = own_embedded[part, :].astype(jnp.float32)
        joined[part, width:] = rms_rows(value, embed_gain[...], width).astype(jnp.bfloat16)
        return carry

    lax.fori_loop(0, 2 * height // slab, norm_inputs, 0)
    def shifted(b, start, size, above):
        value = own_hidden[b * height + start : b * height + start + size, :].astype(jnp.float32)
        value = pltpu.roll(rms_rows(value, hidden_gain[...], width), 1, 0)
        row = lax.broadcasted_iota(jnp.int32, value.shape, 0)
        return jnp.where(row == 0, above, value).astype(jnp.bfloat16)

    for b in range(2):
        joined[b * height : (b + 1) * height, :width] = shifted(b, 0, height, 0.0)

    @pl.when(s == 0)
    def _():
        behind[...] = jnp.zeros_like(behind)

    @pl.when(s > 0)
    def _():
        tail.wait_recv()

    first = rms_rows(behind[...].astype(jnp.float32), hidden_gain[...], width)
    for b in range(2):
        joined[b * height : b * height + 16, :width] = shifted(b, 0, 16, first[b : b + 1, :])
    loads[3].wait()
    mixed[...] = jnp.dot(
        joined[...], proj[...], preferred_element_type=jnp.float32
    ).astype(jnp.bfloat16)
    place_of = pl.ds(pl.multiple_of(v * feature, feature), feature)
    other = pl.ds(pl.multiple_of((1 - c) * height, height), height)
    trade = pltpu.make_async_remote_copy(
        src_ref=mixed.at[other],
        dst_ref=grid.at[count + s, :, place_of],
        send_sem=small_send.at[1],
        recv_sem=small_recv.at[1],
        device_id=place(z, x, y, 1 - c),
        device_id_type=MESH,
    )
    trade.start()
    grid[count + s, :, place_of] = mixed[mine, :]
    trade.wait_recv()
    own_mixed()
    for i in range(SWAPS):
        swap(i).start()
    loads[4].wait()

    served, pairs = plan(depth, pieces, STEPS)
    near = jnp.minimum(z, depth - 1 - z)

    def code_of(head, jz, jx):
        return head * count + jz * 2 + jx

    turns = range(len(pairs[0]))
    codes = [[[code_of(*pairs[k][i][side]) for k in range(len(pairs))] for i in turns] for side in range(2)]
    span = 2 * cols // STEPS
    piece_cols = span // PIECES

    def stat_copy(head, at, i):
        return pltpu.make_async_remote_copy(
            src_ref=packed.at[head * count + at],
            dst_ref=gathered.at[head, c * count * 2 + s * 2 + y],
            send_sem=stat_send.at[head],
            recv_sem=stat_recv.at[head],
            device_id=(at, lax.rem(v + i, vocab)),
            device_id_type=MESH,
        )

    def unit(step, carry):
        turn, sub = step // STEPS, lax.rem(step, STEPS)
        blocks = []
        for side in range(2):
            code = pick([pick(entry, near) for entry in codes[side]], turn)
            head, jz, jx = code // count, lax.rem(code, count) // 2, lax.rem(code, 2)
            blocks.append((head, line_rank(z, depth, jz) * 2 + lax.rem(x + jx, 2)))
        for k, events in enumerate(served):

            @pl.when(near == k)
            def _(k=k, events=events):
                for at_step in sorted({event[0] for event in events}):

                    @pl.when(step == at_step)
                    def _(at_step=at_step):
                        for when, *event in events:
                            if when == at_step:
                                serve(*event)

                @pl.when(sub == 0)
                def _():
                    for i, pair in enumerate(pairs[k]):

                        @pl.when(turn == i)
                        def _(pair=pair):
                            for block in pair:
                                before = [other for both in pairs[k] for other in both]
                                before = before[: before.index(block)]
                                leaves(*block, (1 - block[0], *block[1:]) in before)

        @pl.when(step == 0)
        def _():
            for i in range(SWAPS):
                swap(i).wait_recv()

        @pl.when(sub == 0)
        def _():
            for side, (head, at) in enumerate(blocks):
                gain = jnp.where(head == 0, main_gain[...], mtp_gain[...])

                def norm(i, carry, side=side, head=head, at=at, gain=gain):
                    part = pl.ds(pl.multiple_of(i * slab, slab), slab)
                    value = grid[head * count + at, part, :].astype(jnp.float32)
                    to = pl.ds(pl.multiple_of(side * height + i * slab, slab), slab)
                    rows[to, :] = rms_rows(value, gain, width).astype(jnp.bfloat16)
                    return carry

                lax.fori_loop(0, height // slab, norm, 0)
                want[:, side * height : (side + 1) * height] = wanted[at]
            highs[...] = jnp.full_like(highs, -1e30)
            sums[...] = jnp.zeros_like(sums)
            picks[...] = jnp.zeros_like(picks)

        begin = sub * span
        sublane = lax.broadcasted_iota(jnp.int32, want.shape, 0)
        relative = want[...] - sublane - (s * vocab + y * 2) * cols - begin
        high, total, picked = highs[...], sums[...], picks[...]
        for start in range(0, span, piece_cols):
            columns = pl.ds(pl.multiple_of(begin + start, 16), piece_cols)
            logits = lax.dot_general(
                wide[columns, :], rows[...], ROWS, preferred_element_type=jnp.float32
            )
            tiles = logits.reshape(piece_cols // 8, 8, 2 * height)
            higher = jnp.maximum(high, jnp.max(tiles, axis=0))
            total = total * jnp.exp(high - higher) + jnp.sum(jnp.exp(tiles - higher[None]), axis=0)
            ids = lax.broadcasted_iota(jnp.int32, tiles.shape, 0) * 8 + start
            picked = picked + jnp.sum(jnp.where(relative[None] == ids, tiles, 0.0), axis=0)
            high = higher
        highs[...], sums[...], picks[...] = high, total, picked

        @pl.when(sub == STEPS - 1)
        def _():
            top = jnp.max(high, axis=0, keepdims=True)
            added = jnp.sum(total * jnp.exp(high - top), axis=0, keepdims=True)
            found = jnp.sum(picked, axis=0, keepdims=True)
            block = jnp.where(sublane == 0, top, jnp.where(sublane == 1, added, found))
            for side, (head, at) in enumerate(blocks):
                packed[head * count + at] = block[:, side * height : (side + 1) * height]
            for head, at in blocks:
                for i in range(1, vocab):
                    stat_copy(head, at, i).start()

                @pl.when(at != s)
                def _(head=head, at=at):
                    stat_copy(head, at, 0).start()

                @pl.when(at == s)
                def _(head=head, at=at):
                    pltpu.make_async_copy(
                        packed.at[head * count + at],
                        gathered.at[head, c * count * 2 + s * 2 + y],
                        stat_recv.at[head],
                    ).start()

        return carry

    lax.fori_loop(0, STEPS * len(pairs[0]), unit, 0)

    pl.when(s + 1 < count)(tail.wait_send)
    for i in range(SWAPS):
        swap(i).wait_send()
    trade.wait_send()
    for kind, over_x, over_y, on_z in (
        ("a", 1, count - 1, 2),
        ("b", depth, 0, 1),
        ("ids", depth, 0, 1),
        ("t", 2 * depth, depth, 1),
    ):
        sent(kind, 2, over_x)
        if over_y:
            sent(kind, 3, over_y)
        for k in range(depth):

            @pl.when(z == k)
            def _(k=k, kind=kind, on_z=on_z):
                if k + 1 < depth:
                    sent(kind, 0, on_z * (k + 1))
                if k > 0:
                    sent(kind, 1, on_z * (depth - k))

    for head in range(2):
        others = gathered.at[head, pl.ds(0, devices - 1)]
        pltpu.make_async_copy(others, others, stat_send.at[head]).wait()

    lengths_of = [lengths[0], lengths[1]]
    position = s * height + lax.broadcasted_iota(jnp.int32, (1, height), 1)
    loss = [[None, None], [None, None]]
    group = count * 2
    for head in range(2):
        whole = gathered.at[head]
        pltpu.make_async_copy(whole, whole, stat_recv.at[head]).wait()
        for b in range(2):
            part = gathered[head, b * group : (b + 1) * group, 0:3, :]
            tops = part[:, 0, :]
            top = jnp.max(tops, axis=0, keepdims=True)
            added = jnp.sum(part[:, 1, :] * jnp.exp(tops - top), axis=0, keepdims=True)
            found = jnp.sum(part[:, 2, :], axis=0, keepdims=True)
            loss[head][b] = top + jnp.log(added) - found
    lines = [jnp.zeros((1, height), jnp.float32)] * 4
    for b in range(2):
        inside = position + 1 < lengths_of[b]
        keep = [
            jnp.where((main_mask[b : b + 1, :] == 1) & inside, 1.0, 0.0),
            jnp.where((mtp_mask[b : b + 1, :] == 1) & (position >= 1) & inside, 1.0, 0.0),
        ]
        for head in range(2):
            kept = keep[head] * loss[head][b]
            result[2 * head + b : 2 * head + b + 1, :] = kept
            lines[head] = lines[head] + kept
            lines[2 + head] = lines[2 + head] + keep[head]
    sub = lax.broadcasted_iota(jnp.int32, (8, height), 0)
    tile = jnp.zeros((8, height), jnp.float32)
    for at, line in enumerate(lines):
        tile = jnp.where(sub == at, line, tile)
    tokens[s] = tile

    def token_copy(i):
        return pltpu.make_async_remote_copy(
            src_ref=tokens.at[s],
            dst_ref=tokens.at[s],
            send_sem=small_send.at[2],
            recv_sem=small_recv.at[2],
            device_id=(lax.rem(s + i, count), v),
            device_id_type=MESH,
        )

    for i in range(1, count):
        token_copy(i).start()
    others = tokens.at[pl.ds(0, count - 1)]
    pltpu.make_async_copy(others, others, small_recv.at[2]).wait()
    added = tokens[0]
    for i in range(1, count):
        added = added + tokens[i]
    added = jnp.sum(added, axis=1, keepdims=True)
    main_mean = added[0:1] / jnp.maximum(added[2:3], 1.0)
    mtp_mean = added[1:2] / jnp.maximum(added[3:4], 1.0)
    spot = lax.broadcasted_iota(jnp.int32, (4, height), 0) + lax.broadcasted_iota(jnp.int32, (4, height), 1)
    result[4:8, :] = jnp.where(spot == 0, main_mean + MTP_WEIGHT * mtp_mean, 0.0)

    pltpu.make_async_copy(others, others, small_send.at[2]).wait()


def fused(
    hidden,
    embedded,
    targets,
    main_mask,
    mtp_mask,
    lengths,
    head_weight,
    projection,
    main_gain,
    hidden_gain,
    embed_gain,
    mtp_gain,
):
    batches, seq_len, width = hidden.shape
    count, vocab = lax.axis_size("seq"), lax.axis_size("vocab")
    cols, feature = head_weight.shape[1], projection.shape[1]
    rows = batches * seq_len
    height = rows // 2
    split = height - height // SHARE
    pieces = {
        "a": (0, split * width, "xzy"),
        "b": (0, 2 * (height - split) * width, "zx"),
        "t": (1, height * width, "zyx"),
    }
    memory = pl.BlockSpec(memory_space=pl.ANY)
    local = pl.BlockSpec(memory_space=pltpu.VMEM)
    scalar = pl.BlockSpec(memory_space=pltpu.SMEM)
    chunks = count * 6
    result = pl.pallas_call(
        functools.partial(fused_kernel, (count // 2, split, pieces)),
        out_shape=jax.ShapeDtypeStruct((8, height), jnp.float32),
        in_specs=[memory] * 4 + [local] * 3 + [scalar] + [local] * 4,
        out_specs=local,
        scratch_shapes=[
            pltpu.VMEM((2 * count, height, width), jnp.bfloat16),
            pltpu.VMEM((2 * cols, width), jnp.bfloat16),
            pltpu.VMEM((2 * width, feature), jnp.bfloat16),
            pltpu.VMEM((rows, width), jnp.bfloat16),
            pltpu.VMEM((rows, width), jnp.bfloat16),
            pltpu.VMEM((rows, 2 * width), jnp.bfloat16),
            pltpu.VMEM((rows, feature), jnp.bfloat16),
            pltpu.VMEM((batches, width), jnp.bfloat16),
            pltpu.VMEM((batches, width), jnp.bfloat16),
            pltpu.VMEM((count, 8, height), jnp.int32),
            pltpu.VMEM((rows, width), jnp.bfloat16),
            pltpu.VMEM((8, rows), jnp.int32),
            pltpu.VMEM((8, rows), jnp.float32),
            pltpu.VMEM((8, rows), jnp.float32),
            pltpu.VMEM((8, rows), jnp.float32),
            pltpu.VMEM((2 * count, 8, height), jnp.float32),
            pltpu.VMEM((2, count * vocab, 8, height), jnp.float32),
            pltpu.VMEM((count, 8, height), jnp.float32),
            pltpu.SemaphoreType.DMA((5,)),
            pltpu.SemaphoreType.DMA((len(KINDS), 4)),
            pltpu.SemaphoreType.DMA((chunks,)),
            pltpu.SemaphoreType.DMA((3,)),
            pltpu.SemaphoreType.DMA((3,)),
            pltpu.SemaphoreType.DMA((2,)),
            pltpu.SemaphoreType.DMA((2,)),
            pltpu.SemaphoreType.DMA((SWAPS,)),
            pltpu.SemaphoreType.DMA((SWAPS,)),
        ],
        compiler_params=pltpu.CompilerParams(
            collective_id=0, has_side_effects=True, vmem_limit_bytes=60 * 2**20
        ),
    )(
        hidden.reshape(rows, width),
        embedded.reshape(rows, width),
        head_weight.T,
        projection,
        targets,
        main_mask,
        mtp_mask,
        lengths,
        main_gain.reshape(1, -1),
        hidden_gain.reshape(1, -1),
        embed_gain.reshape(1, -1),
        mtp_gain.reshape(1, -1),
    )
    return result[0:2], result[2:4], jnp.sum(result[4:6])


def program(hidden, embedded, targets, *rest):
    one_tile = hidden.shape[0] == 2 and hidden.shape[1] == 128 and rest[3].shape[1] % (8 * STEPS * PIECES) == 0
    if lax.axis_size("vocab") == 4 and one_tile:
        return fused(hidden, embedded, targets, *rest)
    return shards(hidden, embedded, targets, *rest)


def solution(mesh):
    return jax.shard_map(
        program,
        mesh=mesh,
        in_specs=(
            P(None, "seq", None),
            P(None, "seq", None),
            P(None, "seq"),
            P(None, "seq"),
            P(None, "seq"),
            P(),
            P(None, ("seq", "vocab")),
            P(None, "vocab"),
            P(),
            P(),
            P(),
            P(),
        ),
        out_specs=(P(None, "seq"), P(None, "seq"), P()),
        check_vma=False,
    )
```
